256 devices in a mesh: dp: 64 (over x, z, core), cent: 4 (over y).
Axes of the slice: x: 4, y: 4, z: 8, core: 2. Of those that a mesh axis runs over, the one named last changes fastest.
Arguments:
- documents: bfloat16 [131072, 2048], P(('dp', 'cent')), may hold values from -6 to 6
- assigned: int32 [131072], P(('dp', 'cent')), may hold values from 0 to 98303, as said below
- centroids: bfloat16 [98304, 2048], P(('dp', 'cent')), may hold values from -6 to 6
- owner_slot: int32 [98304], replicated, may hold values from 0 to 98303, as said below
Outputs:
- prototypicality: float32 [131072], P(('dp', 'cent'))
- redundancy: float32 [131072], P(('dp', 'cent'))
- cluster_stats: float32 [3, 98304], P(None, ('dp', 'cent'))
The draws below stay inside these ranges and needn't reach their ends.
Inputs may be any that keep to these rules, and one draw needn't show every extreme that they name: `owner_slot`: A permutation of the cluster numbers. `assigned`: of the 512 documents of one device, at most 4 have a slot in any one owner's block of 384 slots, and at most 10 have slots with the owners that share one dp index; in every draw some device reaches 10, and one owner receives exactly 4 from every device.
All inputs are finite; a program needn't handle non-finite values.
Results may differ from the reference program's by a relative error of at most 0.0003.
Values may be sent and summed in bfloat16 or wider, within the bound.
A program may use at most 64 MiB of HBM per device.

```python
import jax
import jax.numpy as jnp
from jax import lax

D = 2048
DOC_DEV = 512
CL_DEV = 384
DOCS = 131072
CLUSTERS = 98304
CAP = 4
GCAP = 10
N_CENT = 4
DEVICES = 256


def slot_permutation(key):
    return jax.random.permutation(jax.random.fold_in(key, 11), CLUSTERS).astype(jnp.int32)


def draw_owner_slot(key, part):
    return slot_permutation(key)


def draw_assigned(key, part):
    permuted = slot_permutation(key)
    inverse = jnp.zeros((CLUSTERS,), jnp.int32).at[permuted].set(jnp.arange(CLUSTERS, dtype=jnp.int32))
    base = jax.random.fold_in(key, 23)
    key_forced = jax.random.fold_in(base, 1)
    key_favour = jax.random.fold_in(base, 2)
    key_ticket = jax.random.fold_in(base, 3)
    key_choose = jax.random.fold_in(base, 4)
    key_shuffle = jax.random.fold_in(base, 5)
    key_local = jax.random.fold_in(base, 6)
    row_count = DEVICES // N_CENT
    per_row = N_CENT * CAP
    forced = jax.random.randint(key_forced, (), 0, DEVICES, dtype=jnp.int32)
    forced_row = forced // N_CENT
    forced_col = forced % N_CENT
    row_ids = jnp.arange(row_count, dtype=jnp.int32)[None, :]
    favour = jax.random.randint(key_favour, (DEVICES, row_count), 0, N_CENT, dtype=jnp.int32)
    favour = jnp.where(row_ids == forced_row, forced_col, favour)
    ticket_ids = jnp.arange(per_row, dtype=jnp.int32)
    ticket_col = ticket_ids // CAP
    noise = jax.random.randint(key_ticket, (DEVICES, row_count, per_row), 0, 1 << 19, dtype=jnp.int32)
    boost = jnp.where(ticket_col[None, None, :] == favour[:, :, None], 1 << 29, 0).astype(jnp.int32)
    score = noise * per_row + ticket_ids[None, None, :] + boost
    kept = jnp.argsort(-score, axis=-1)[:, :, :GCAP].astype(jnp.int32)
    kept_owner = row_ids[:, :, None] * N_CENT + kept // CAP
    kept_owner = kept_owner.reshape(DEVICES, row_count * GCAP)
    pool = row_count * GCAP
    pool_ids = jnp.arange(pool, dtype=jnp.int32)
    pool_row = pool_ids // GCAP
    noise_two = jax.random.randint(key_choose, (DEVICES, pool), 0, 1 << 19, dtype=jnp.int32)
    boost_two = jnp.where(pool_row == forced_row, 1 << 29, 0).astype(jnp.int32)
    score_two = noise_two * pool + pool_ids[None, :] + boost_two[None, :]
    chosen = jnp.argsort(-score_two, axis=-1)[:, :DOC_DEV].astype(jnp.int32)
    chosen_owner = jnp.take_along_axis(kept_owner, chosen, axis=1)
    noise_three = jax.random.randint(key_shuffle, (DEVICES, DOC_DEV), 0, 1 << 19, dtype=jnp.int32)
    score_three = noise_three * DOC_DEV + jnp.arange(DOC_DEV, dtype=jnp.int32)[None, :]
    shuffled = jnp.argsort(score_three, axis=-1).astype(jnp.int32)
    final_owner = jnp.take_along_axis(chosen_owner, shuffled, axis=1)
    local_draws = jax.random.randint(key_local, (3, DEVICES, DOC_DEV), 0, CL_DEV, dtype=jnp.int32)
    local_ids = jnp.min(local_draws, axis=0)
    slot_ids = final_owner * CL_DEV + local_ids
    return inverse[slot_ids.reshape(DOCS)]


def block_levels(stream_key, extent, pieces, smallest, high):
    gain, own = 1.0, jax.random.fold_in(stream_key, 6)
    for dim, shards_of in pieces:
        steps = jnp.exp(jax.random.uniform(jax.random.fold_in(own, dim), (shards_of,), jnp.float32, smallest / len(pieces), high / len(pieces)))
        gain = gain * jnp.repeat(steps, extent[dim] // shards_of).reshape([-1 if axis == dim else 1 for axis in range(len(extent))])
    return gain


def normal_values(key, shape, scale, reach, cuts=(), held_as=jnp.bfloat16):
    entries = jax.random.normal(key, shape, jnp.float32) * scale
    if len(cuts) > 0:
        entries = block_levels(key, shape, cuts, -0.22, 0.18) * entries
    return jnp.clip(entries, min=-reach, max=reach).astype(held_as)


def setup_inputs(seed: int = 0) -> dict:
    key_list = jax.random.split(jax.random.key(seed), 5)
    documents = normal_values(key_list[0], (DOCS, D), 1.0, 6.0, ((0, 256),))
    assigned = draw_assigned(jax.random.fold_in(key_list[4], 71), 0)
    centroids = normal_values(key_list[2], (CLUSTERS, D), 1.0, 6.0, ((0, 256),))
    owner_slot = draw_owner_slot(jax.random.fold_in(key_list[4], 71), 0)
    return dict(documents=documents, assigned=assigned, centroids=centroids, owner_slot=owner_slot)


def reference(documents, assigned, centroids, owner_slot):
    slot_ids = owner_slot[assigned]
    owner_ids = slot_ids // CL_DEV
    cent_sq = lax.optimization_barrier(jnp.sum(jnp.square(centroids.astype(jnp.float32)), axis=1))

    def block_sim(packed):
        doc_block, slot_block = packed
        doc_rows = doc_block.astype(jnp.float32)
        cent_rows = centroids[slot_block].astype(jnp.float32)
        cross_dot = lax.optimization_barrier(jnp.sum(doc_rows * cent_rows, axis=1))
        self_sq = lax.optimization_barrier(jnp.sum(doc_rows * doc_rows, axis=1))
        similar = cross_dot * lax.rsqrt(self_sq + 1.0) * lax.rsqrt(cent_sq[slot_block] + 1.0)
        return (similar, self_sq)
    similarity, self_sq = lax.map(block_sim, (documents.reshape(DEVICES, DOC_DEV, D), slot_ids.reshape(DEVICES, DOC_DEV)))
    similarity = similarity.reshape(DOCS)
    self_sq = self_sq.reshape(DOCS)
    counts = jax.ops.segment_sum(jnp.ones((DOCS,), jnp.float32), slot_ids, num_segments=CLUSTERS)
    totals = jax.ops.segment_sum(similarity, slot_ids, num_segments=CLUSTERS)
    squares = jax.ops.segment_sum(similarity * similarity, slot_ids, num_segments=CLUSTERS)
    cluster_stats = jnp.stack([counts, totals, squares])
    count_floor = jnp.maximum(counts, 1.0)
    mean_sim = totals / count_floor
    variance = jnp.maximum(squares / count_floor - mean_sim * mean_sim, 0.0)
    prototypicality = (mean_sim[slot_ids] - similarity) / jnp.sqrt(variance[slot_ids] + 1.0 / D)
    owner_grid = owner_ids.reshape(DEVICES, DOC_DEV)
    is_owner = (owner_grid[:, :, None] == jnp.arange(DEVICES, dtype=jnp.int32)[None, None, :]).astype(jnp.int32)
    rank_ids = lax.optimization_barrier(jnp.sum((jnp.cumsum(is_owner, axis=1) - 1) * is_owner, axis=2)).astype(jnp.int32)
    source_ids = jnp.arange(DEVICES, dtype=jnp.int32)[:, None]
    position = owner_grid * (DEVICES * CAP) + source_ids * CAP + rank_ids
    member_table = jnp.full((DEVICES * DEVICES * CAP,), DOCS, jnp.int32)
    member_table = member_table.at[position.reshape(-1)].set(jnp.arange(DOCS, dtype=jnp.int32))
    member_table = member_table.reshape(DEVICES, DEVICES * CAP)
    inverse_norm = lax.rsqrt(self_sq + 1.0)
    slot_count = DEVICES * CAP
    not_self = jnp.arange(slot_count, dtype=jnp.int32)[:, None] != jnp.arange(slot_count, dtype=jnp.int32)[None, :]

    def owner_redundancy(members):
        is_live = members < DOCS
        safe_ids = jnp.minimum(members, DOCS - 1)
        doc_rows = documents[safe_ids].astype(jnp.float32)
        gram_block = jnp.dot(doc_rows, doc_rows.T, precision=lax.Precision.HIGHEST)
        row_scale = jnp.where(is_live, inverse_norm[safe_ids], 0.0)
        cosine = gram_block * row_scale[:, None] * row_scale[None, :]
        cluster_tag = jnp.where(is_live, slot_ids[safe_ids], -1)
        same_cluster = (cluster_tag[:, None] == cluster_tag[None, :]) & is_live[:, None] & not_self
        return jnp.sqrt(jnp.float32(D)) * lax.optimization_barrier(jnp.max(jnp.where(same_cluster, cosine, 0.0), axis=1))
    redundant = lax.map(owner_redundancy, member_table)
    redundancy = jnp.zeros((DOCS,), jnp.float32).at[member_table.reshape(-1)].set(redundant.reshape(-1), mode='drop')
    return (prototypicality, redundancy, cluster_stats)
```

```python
import math

import jax
import jax.numpy as jnp
from jax import lax
from jax.experimental import pallas as pl
from jax.experimental.pallas import tpu as pltpu
from jax.sharding import Mesh
from jax.sharding import PartitionSpec as P

AXES = ("dp_0", "dp_1", "dp_2", "cent")
MESH = pl.DeviceIdType.MESH
F32 = jnp.float32
BF16 = jnp.bfloat16
HIGHEST = lax.Precision.HIGHEST

NX, NZ, NK, NY = 4, 8, 2, 4
NJ = NX * NK
GROUPS = NZ * NJ
MAIN, SPILL, CAP = 8, 2, 4
STEPS = (0, 4, 3, 5, 2, 6, 1, 7)
ROWS = NJ * CAP
BLOCK = NY * ROWS


def dot(a, b, dims=((1,), (0,)), precision=None):
    return lax.dot_general(a, b, (dims, ((), ())), precision=precision, preferred_element_type=F32)


def iota(shape, dim):
    return lax.broadcasted_iota(jnp.int32, shape, dim)


def fiota(shape, dim):
    return iota(shape, dim).astype(F32)


def rsum(value, axis):
    return jnp.sum(value, axis=axis, keepdims=True)


def rmax(value, axis):
    return jnp.max(value, axis=axis, keepdims=True)


def one_if(mask, dtype=F32):
    return jnp.where(mask, 1.0, 0.0).astype(dtype)


def kernel(
    slot_ref, docs_hbm, cents_hbm,
    proto_ref, red_ref, stats_ref,
    docs, cents, out, inbox, fwd, block,
    tag_out, tag_in, own_out, own_in,
    assign, place, qcol, tags, rowscale, rowtag, simil, best, rowbest, tot,
    score, score_in, reply, reply_in,
    load_sem, doc_send, doc_recv, tag_send, tag_recv, own_send, own_recv,
    fwd_send, fwd_recv, score_send, score_recv, reply_send, reply_recv,
):
    x, z, k, y = (lax.axis_index(a) for a in AXES)
    count, width = docs.shape
    table = cents.shape[0]
    quarter = width // 4
    me_j = x * NK + k

    load_docs = pltpu.make_async_copy(docs_hbm, docs, load_sem.at[0])
    load_cents = pltpu.make_async_copy(cents_hbm, cents, load_sem.at[1])
    load_docs.start()
    load_cents.start()

    def peer(dz, t):
        px = lax.rem(x + t // NK, NX)
        pk = lax.rem(k + lax.rem(t, NK), NK)
        pz = lax.rem(z + dz, NZ)
        return px, pz, pk

    barrier = pltpu.get_barrier_semaphore()

    def greet(t, carry):
        px, pz, pk = peer(t // NJ, lax.rem(t, NJ))
        pl.semaphore_signal(barrier, inc=1, device_id=(px, pz, pk, y), device_id_type=MESH)
        return carry

    lax.fori_loop(1, GROUPS, greet, 0)
    for dy in range(1, NY):
        pl.semaphore_signal(
            barrier, inc=1, device_id=(x, z, k, lax.rem(y + dy, NY)), device_id_type=MESH
        )

    slot = slot_ref[...].astype(F32)
    owner = jnp.floor((slot + 0.5) * (1.0 / table))
    local = slot - owner * table
    row = jnp.floor(owner * (1.0 / NY))
    col = owner - row * NY
    dest_x = jnp.floor(row * (1.0 / (NZ * NK)))
    rest = row - dest_x * (NZ * NK)
    dest_z = jnp.floor(rest * (1.0 / NK))
    dest_k = rest - dest_z * NK
    step = dest_z - z.astype(F32)
    step = jnp.where(step < 0.0, step + NZ, step)
    order = jnp.zeros_like(step)
    for n, dz in enumerate(STEPS):
        order = jnp.where(step == float(dz), float(n), order)
    col = col - y.astype(F32)
    col = jnp.where(col < 0.0, col + NY, col)
    group = order * NJ + dest_x * NK + dest_k
    at_group = one_if(fiota((GROUPS, count), 0) == group)
    at_owner = one_if(fiota((GROUPS * NY, count), 0) == group * NY + col)
    earlier = one_if(iota((count, count), 0) < iota((count, count), 1), BF16)
    rank = rsum(dot(at_group.astype(BF16), earlier) * at_group, 0)
    rank_owner = rsum(dot(at_owner.astype(BF16), earlier) * at_owner, 0)
    is_main = rank < float(MAIN)
    main_at = jnp.where(is_main, group * MAIN + rank, -1.0)
    spill_at = jnp.where(is_main, -8.0, group * MAIN + (rank - MAIN) * 4.0)
    assign[...] = at_group
    place[...] = col * (2.0 * CAP) + rank_owner

    jf = me_j.astype(F32)
    value = col * float(ROWS) + jf * CAP + rank_owner + 1.0
    lane = fiota((128, count), 0)
    main_lane = jnp.where(is_main, jf * MAIN + rank, -8.0)
    spill_lane = jnp.where(is_main, -8.0, 64.0 + jf * MAIN + (rank - MAIN) * 4.0)
    hit = (lane == main_lane) | ((lane >= spill_lane) & (lane < spill_lane + 4.0))
    first = dot(at_group.astype(BF16), jnp.where(hit, value, 0.0).astype(BF16), ((1,), (1,)))
    hit = lane == value - 1.0
    high = jnp.floor((local + 1.0) * (1.0 / 16.0))
    low = local + 1.0 - high * 16.0
    second = 16.0 * dot(at_group.astype(BF16), jnp.where(hit, high, 0.0).astype(BF16), ((1,), (1,)))
    second += dot(at_group.astype(BF16), jnp.where(hit, low, 0.0).astype(BF16), ((1,), (1,)))
    both = jnp.concatenate([first, second], axis=1)
    for g in range(GROUPS):
        tag_out[g] = both[g : g + 1, :]
    tag_in[me_j] = tag_out[me_j]

    load_docs.wait()

    half = GROUPS // 2

    def pack(h):
        at = fiota((half * MAIN, count), 0) + float(h * half * MAIN)
        pick = one_if(at == main_at, BF16)
        for q in range(4):
            cols = slice(q * quarter, (q + 1) * quarter)
            packed = dot(pick, docs[:, cols]).astype(BF16)
            out[h * half : (h + 1) * half, :, cols] = packed.reshape(half, MAIN, quarter)
        spilled = jnp.zeros((half * MAIN, quarter), F32)
        for q in range(4):
            cols = slice(q * quarter, (q + 1) * quarter)
            spilled += dot(one_if(at == spill_at + float(q), BF16), docs[:, cols])
        out[h * half : (h + 1) * half, :, width:] = spilled.astype(BF16).reshape(half, MAIN, quarter)

    def send_docs(n):
        dz = STEPS[n]

        def body(t, carry):
            px, pz, pk = peer(dz, t)
            pltpu.make_async_remote_copy(
                src_ref=out.at[n * NJ + px * NK + pk],
                dst_ref=inbox.at[n * NJ + me_j],
                send_sem=doc_send.at[n],
                recv_sem=doc_recv.at[n],
                device_id=(px, pz, pk, y),
                device_id_type=MESH,
            ).start()
            return carry

        lax.fori_loop(1 if dz == 0 else 0, NJ, body, 0)

    def arrived(ref, sem):
        pltpu.make_async_copy(ref, ref, sem).wait()

    def y_send(dy, src, dst, send, recv):
        return pltpu.make_async_remote_copy(
            src_ref=src, dst_ref=dst, send_sem=send, recv_sem=recv,
            device_id=(x, z, k, lax.rem(y + dy, NY)), device_id_type=MESH,
        )

    pack(0)
    pl.semaphore_wait(barrier, GROUPS - 1 + NY - 1)

    for n, dz in enumerate(STEPS):

        def send_tag(t, carry, n=n, dz=dz):
            px, pz, pk = peer(dz, t)
            pltpu.make_async_remote_copy(
                src_ref=tag_out.at[n * NJ + px * NK + pk],
                dst_ref=tag_in.at[n * NJ + me_j],
                send_sem=tag_send,
                recv_sem=tag_recv,
                device_id=(px, pz, pk, y),
                device_id_type=MESH,
            ).start()
            return carry

        lax.fori_loop(1 if dz == 0 else 0, NJ, send_tag, 0)

    for n in range(NZ // 2):
        send_docs(n)
    inbox[me_j] = out[me_j]
    pack(1)
    load_cents.wait()

    squares = jnp.zeros((table, 128), F32)
    for c in range(width // 128):
        part = cents[:, c * 128 : (c + 1) * 128].astype(F32)
        squares += part * part
    qcol[...] = lax.rsqrt(rsum(squares, 1) + 1.0)

    for n in range(NZ // 2, NZ):
        send_docs(n)

    arrived(tag_in.at[pl.ds(0, GROUPS - 1)], tag_recv)
    for n in range(NZ):
        own = tag_in[n * NJ]
        for j in range(1, NJ):
            own += tag_in[n * NJ + j]
        own_out[n : n + 1, :] = own
    for dy in range(1, NY):
        y_send(dy, own_out, own_in.at[dy], own_send, own_recv).start()
    own_in[0] = own_out[...]

    tot[...] = jnp.zeros_like(tot)
    best[...] = jnp.zeros_like(best)
    rowbest[...] = jnp.zeros_like(rowbest)

    def relay(n, in_groups):
        in_groups()
        marks = own_out[pl.ds(n, 1), :]
        target = fiota((BLOCK, 64), 0) + 1.0
        pick = one_if(target == marks[:, :64], BF16)
        spill = target == marks[:, 64:128]
        phase = lax.rem(iota((BLOCK, 64), 1), 4)
        got = inbox[pl.ds(n * NJ, NJ)].reshape(64, width + quarter)
        for q in range(4):
            cols = slice(q * quarter, (q + 1) * quarter)
            rows = dot(pick, got[:, cols])
            rows += dot(one_if(spill & (phase == q), BF16), got[:, width:])
            rows = rows.astype(BF16)
            block[n, :ROWS, cols] = rows[:ROWS]
            fwd[n, :, cols] = rows[ROWS:]
        for dy in range(1, NY):
            y_send(
                dy,
                fwd.at[n, pl.ds((dy - 1) * ROWS, ROWS)],
                block.at[n, pl.ds(dy * ROWS, ROWS)],
                fwd_send.at[n],
                fwd_recv.at[n],
            ).start()

    eye = iota((BLOCK, BLOCK), 0) == iota((BLOCK, BLOCK), 1)
    source = iota((NZ, 128), 1) // ROWS

    def owner_block(n):
        arrived(block.at[n, pl.ds(0, BLOCK - ROWS)], fwd_recv.at[n])
        mine = block[n]
        tag = tags[pl.ds(n, 1), :]
        gram = dot(mine, mine, ((1,), (1,)))
        square = jnp.where(eye, gram, 0.0)
        scale = lax.rsqrt(rsum(square, 0) + 1.0)
        scale_col = lax.rsqrt(rsum(square, 1) + 1.0)
        tag_col = rsum(jnp.where(eye, jnp.broadcast_to(tag, (BLOCK, BLOCK)), 0.0), 1)
        rowscale[n] = jnp.broadcast_to(scale_col, (BLOCK, BLOCK))
        rowtag[n] = jnp.broadcast_to(tag_col, (BLOCK, BLOCK))
        live = tag > 0.0
        pair = jnp.where((tag_col == tag) & live & jnp.logical_not(eye), gram, 0.0)
        top = rmax(pair * scale_col, 0)

        def earlier_block(m, top):
            other = dot(block[m], mine, ((1,), (1,)))
            pair = jnp.where((rowtag[m] == tag) & live, other, 0.0)
            rowbest[m] = jnp.maximum(rowbest[m], pair * scale)
            return jnp.maximum(top, rmax(pair * rowscale[m], 0))

        top = lax.fori_loop(0, n, earlier_block, top)
        best[pl.ds(n, 1), :] = top * scale

        cross = dot(cents[...], mine, ((1,), (1,)))
        member = (fiota((table, BLOCK), 0) + 1.0) == tag
        similar = rsum(jnp.where(member, cross * qcol[...], 0.0), 0) * scale
        simil[pl.ds(n, 1), :] = similar
        tot[0] += one_if(member)
        tot[1] += jnp.where(member, similar, 0.0)
        tot[2] += jnp.where(member, similar * similar, 0.0)

    def doc_wait(n, count):
        arrived(inbox.at[pl.ds(0, count)], doc_recv.at[n])

    relay(0, lambda: doc_wait(0, NJ - 1))
    arrived(own_in.at[pl.ds(1, NY - 1)], own_recv)
    mix = jnp.zeros((NZ, 128), F32)
    for dy in range(NY):
        mix = jnp.where(source == dy, own_in[dy, :, 128:], mix)
    tags[...] = mix

    def main_step(n, carry):
        relay(n, lambda: doc_wait(n, NJ))
        owner_block(n - 1)
        return carry

    lax.fori_loop(1, NZ, main_step, 0)
    owner_block(NZ - 1)

    counts = rsum(tot[0], 1)
    sums = rsum(tot[1], 1)
    squares = rsum(tot[2], 1)
    pos = iota((table, 128), 1)
    stacked = jnp.where(pos == 0, counts, jnp.where(pos == 1, sums, jnp.where(pos == 2, squares, 0.0)))
    stats_ref[...] = stacked.T[:3]
    floor = jnp.maximum(counts, 1.0)
    mean = sums / floor
    spread = jnp.sqrt(jnp.maximum(squares / floor - mean * mean, 0.0) + 1.0 / width)

    def scores(n, carry):
        tag = tags[pl.ds(n, 1), :]
        member = (fiota((table, BLOCK), 0) + 1.0) == tag
        mean_at = rsum(jnp.where(member, mean, 0.0), 0)
        spread_at = rsum(jnp.where(member, spread, 0.0), 0)
        gap = (mean_at - simil[pl.ds(n, 1), :]) / jnp.where(tag > 0.0, spread_at, 1.0)
        score[0, pl.ds(n, 1), :] = jnp.where(tag > 0.0, gap, 0.0)
        rows = rmax((rowbest[n] * rowscale[n]).T, 0)
        score[1, pl.ds(n, 1), :] = math.sqrt(width) * jnp.maximum(best[pl.ds(n, 1), :], rows)
        return carry

    lax.fori_loop(0, NZ, scores, 0)
    for dy in range(1, NY):
        y_send(NY - dy, score, score_in.at[dy], score_send, score_recv).start()
    score_in[0] = score[...]

    arrived(score_in.at[pl.ds(1, NY - 1)], score_recv)
    lanes = iota((GROUPS, 128), 1)
    mine = lax.rem(lanes, ROWS) // CAP == lax.rem(iota((GROUPS, 128), 0), NJ)
    from_lane, to_lane = iota((128, 128), 0), iota((128, 128), 1)
    laid = jnp.zeros((GROUPS, 128), F32)
    for s in range(2):
        held = jnp.zeros((NZ, 128), F32)
        for dy in range(NY):
            held = jnp.where(source == dy, score_in[dy, s], held)
        held = jnp.broadcast_to(held[:, None, :], (NZ, NJ, 128)).reshape(GROUPS, 128)
        move = one_if(to_lane == (from_lane // ROWS) * (2 * CAP) + s * CAP + lax.rem(from_lane, CAP))
        laid += dot(jnp.where(mine, held, 0.0), move, precision=HIGHEST)
    for g in range(GROUPS):
        reply[g] = laid[g : g + 1, :]

    for n, dz in enumerate(STEPS):

        def send_reply(t, carry, n=n, dz=dz):
            px, pz, pk = peer(NZ - dz, t)
            pltpu.make_async_remote_copy(
                src_ref=reply.at[n * NJ + px * NK + pk],
                dst_ref=reply_in.at[n * NJ + me_j],
                send_sem=reply_send,
                recv_sem=reply_recv,
                device_id=(px, pz, pk, y),
                device_id_type=MESH,
            ).start()
            return carry

        lax.fori_loop(1 if dz == 0 else 0, NJ, send_reply, 0)
    reply_in[me_j] = reply[me_j]
    arrived(reply_in.at[pl.ds(0, GROUPS - 1)], reply_recv)
    home = jnp.concatenate(
        [reply_in[...].reshape(GROUPS, 128), jnp.zeros((128 - GROUPS, 128), F32)], axis=0
    ).T
    picked = dot(home[: NY * 2 * CAP, :GROUPS], assign[...], precision=HIGHEST)
    at = fiota((NY * 2 * CAP, count), 0)
    proto_ref[...] = rsum(jnp.where(at == place[...], picked, 0.0), 0)
    red_ref[...] = rsum(jnp.where(at == place[...] + CAP, picked, 0.0), 0)

    for n, dz in enumerate(STEPS):
        arrived(inbox.at[pl.ds(0, NJ - 1 if dz == 0 else NJ)], doc_send.at[n])
        arrived(fwd.at[n], fwd_send.at[n])
    arrived(tag_out.at[pl.ds(0, GROUPS - 1)], tag_send)
    arrived(reply.at[pl.ds(0, GROUPS - 1)], reply_send)
    arrived(own_in.at[pl.ds(1, NY - 1)], own_send)
    arrived(score_in.at[pl.ds(1, NY - 1)], score_send)


def local(documents, assigned, centroids, owner_slot):
    count, width = documents.shape
    table = centroids.shape[0]
    wide = width + width // 4
    slot = owner_slot[assigned].reshape(1, count)
    dma = pltpu.SemaphoreType.DMA
    proto, red, stats = pl.pallas_call(
        kernel,
        out_shape=(
            jax.ShapeDtypeStruct((1, count), F32),
            jax.ShapeDtypeStruct((1, count), F32),
            jax.ShapeDtypeStruct((3, table), F32),
        ),
        in_specs=[
            pl.BlockSpec(memory_space=pltpu.VMEM),
            pl.BlockSpec(memory_space=pl.ANY),
            pl.BlockSpec(memory_space=pl.ANY),
        ],
        out_specs=(pl.BlockSpec(memory_space=pltpu.VMEM),) * 3,
        scratch_shapes=[
            pltpu.VMEM((count, width), BF16),
            pltpu.VMEM((table, width), BF16),
            pltpu.VMEM((GROUPS, MAIN, wide), BF16),
            pltpu.VMEM((GROUPS, MAIN, wide), BF16),
            pltpu.VMEM((NZ, BLOCK - ROWS, width), BF16),
            pltpu.VMEM((NZ, BLOCK, width), BF16),
            pltpu.VMEM((GROUPS, 1, 256), F32),
            pltpu.VMEM((GROUPS, 1, 256), F32),
            pltpu.VMEM((NZ, 256), F32),
            pltpu.VMEM((NY, NZ, 256), F32),
            pltpu.VMEM((GROUPS, count), F32),
            pltpu.VMEM((1, count), F32),
            pltpu.VMEM((table, 1), F32),
            pltpu.VMEM((NZ, BLOCK), F32),
            pltpu.VMEM((NZ, BLOCK, BLOCK), F32),
            pltpu.VMEM((NZ, BLOCK, BLOCK), F32),
            pltpu.VMEM((NZ, BLOCK), F32),
            pltpu.VMEM((NZ, BLOCK), F32),
            pltpu.VMEM((NZ, BLOCK, BLOCK), F32),
            pltpu.VMEM((3, table, BLOCK), F32),
            pltpu.VMEM((2, NZ, BLOCK), F32),
            pltpu.VMEM((NY, 2, NZ, BLOCK), F32),
            pltpu.VMEM((GROUPS, 1, 128), F32),
            pltpu.VMEM((GROUPS, 1, 128), F32),
            dma((2,)),
            dma((NZ,)), dma((NZ,)),
            dma, dma,
            dma, dma,
            dma((NZ,)), dma((NZ,)),
            dma, dma,
            dma, dma,
        ],
        compiler_params=pltpu.CompilerParams(
            collective_id=0, has_side_effects=True, vmem_limit_bytes=56 * 1024 * 1024
        ),
        name="route_and_score",
    )(slot, documents, centroids)
    return proto.reshape(count), red.reshape(count), stats


def solution(mesh):
    split = Mesh(mesh.devices.reshape(NX, NZ, NK, NY), AXES)
    placed = (P(AXES, None), P(AXES), P(AXES, None), P())
    return jax.shard_map(
        local,
        mesh=split,
        in_specs=placed,
        out_specs=(P(AXES), P(AXES), P(None, AXES)),
        check_vma=False,
    )
```

```python
import math

import jax
import jax.numpy as jnp
from jax import lax
from jax.experimental import pallas as pl
from jax.experimental.pallas import tpu as pltpu
from jax.sharding import Mesh
from jax.sharding import PartitionSpec as P

AXES = ("dp_0", "dp_1", "dp_2", "cent")
MESH = pl.DeviceIdType.MESH
F32 = jnp.float32
BF16 = jnp.bfloat16
HIGHEST = lax.Precision.HIGHEST

NX, NZ, NK, NY = 4, 8, 2, 4
NJ = NX * NK
GROUPS = NZ * NJ
MAIN, SPILL, CAP = 8, 2, 4
STEPS = tuple((n + 1) // 2 if n % 2 else -(n // 2) % NZ for n in range(NZ))
ROWS = NJ * CAP
BLOCK = NY * ROWS


def dot(a, b, dims=((1,), (0,)), precision=None):
    return lax.dot_general(a, b, (dims, ((), ())), precision=precision, preferred_element_type=F32)


def iota(shape, dim):
    return lax.broadcasted_iota(jnp.int32, shape, dim)


def fiota(shape, dim):
    return iota(shape, dim).astype(F32)


def rsum(value, axis):
    return jnp.sum(value, axis=axis, keepdims=True)


def rmax(value, axis):
    return jnp.max(value, axis=axis, keepdims=True)


def one_if(mask, dtype=F32):
    return jnp.where(mask, 1.0, 0.0).astype(dtype)


def kernel(
    assigned_hbm, slots_hbm, docs_hbm, cents_hbm,
    reply_in, assign, place, stats_ref,
    assigned, slots, docs, cents, out, inbox, fwd, block,
    tag_out, tag_in, own_out, own_in,
    qcol, tags, rowscale, rowtag, simil, best, rowbest, tot,
    score, score_in, reply,
    ring, load_sem, doc_send, doc_recv, tag_send, tag_recv, own_send, own_recv,
    fwd_send, fwd_recv, score_send, score_recv, reply_send, reply_recv,
):
    x, z, k, y = (lax.axis_index(a) for a in AXES)
    count, width = docs.shape
    table = cents.shape[0]
    quarter = width // 4

    load_assigned = pltpu.make_async_copy(assigned_hbm, assigned, load_sem.at[2])
    load_slots = pltpu.make_async_copy(slots_hbm, slots, load_sem.at[3])
    load_docs = pltpu.make_async_copy(docs_hbm, docs, load_sem.at[0])
    load_cents = pltpu.make_async_copy(cents_hbm, cents, load_sem.at[1])
    load_assigned.start()
    load_slots.start()
    load_docs.start()
    load_cents.start()

    def peer(dz, t, sign=1):
        px = lax.rem(x + NX + sign * (t // NK), NX)
        pk = lax.rem(k + NK + sign * lax.rem(t, NK), NK)
        pz = lax.rem(z + NZ + sign * dz, NZ)
        return px, pz, pk

    barrier = pltpu.get_barrier_semaphore()

    def hello(sem, px, pz, pk, py):
        pl.semaphore_signal(sem, inc=1, device_id=(px, pz, pk, py), device_id_type=MESH)

    above, below = lax.rem(z + 1, NZ), lax.rem(z + NZ - 1, NZ)
    hello(barrier, x, above, k, y)
    hello(barrier, x, below, k, y)
    for t in range(1, NJ):
        px, pz, pk = peer(0, t)
        hello(barrier, px, pz, pk, y)
    for dy in range(1, NY):
        hello(barrier, x, z, k, lax.rem(y + dy, NY))

    def ring_signal(r):
        hello(ring.at[r, 0], x, above, k, y)
        hello(ring.at[r, 1], x, below, k, y)

    def ring_wait(r):
        pl.semaphore_wait(ring.at[r, 0], 1)
        pl.semaphore_wait(ring.at[r, 1], 1)

    load_assigned.wait()
    load_slots.wait()
    number = assigned[...].astype(F32)
    at_row = jnp.floor(number * (1.0 / 128.0))
    at_lane = number - at_row * 128.0
    held = slots.shape[0]
    turned = jnp.concatenate(
        [slots[r * 128 : (r + 1) * 128, :].astype(F32).T for r in range(held // 128)], axis=1
    )
    top = jnp.floor(turned * (1.0 / 4096.0))
    turned -= top * 4096.0
    middle = jnp.floor(turned * (1.0 / 64.0))
    turned -= middle * 64.0
    digits = jnp.concatenate([top, middle, turned], axis=0).astype(BF16)
    digits = dot(digits, one_if(fiota((held, count), 0) == at_row, BF16))
    slot = digits[:128] * 4096.0 + digits[128:256] * 64.0 + digits[256:]
    slot = rsum(jnp.where(fiota((128, count), 0) == at_lane, slot, 0.0), 0)

    owner = jnp.floor((slot + 0.5) * (1.0 / table))
    local = slot - owner * table
    row = jnp.floor(owner * (1.0 / NY))
    col = owner - row * NY
    dest_x = jnp.floor(row * (1.0 / (NZ * NK)))
    rest = row - dest_x * (NZ * NK)
    dest_z = jnp.floor(rest * (1.0 / NK))
    dest_k = rest - dest_z * NK
    step = dest_z - z.astype(F32)
    step = jnp.where(step < 0.0, step + NZ, step)
    order = jnp.zeros_like(step)
    for n, dz in enumerate(STEPS):
        order = jnp.where(step == float(dz), float(n), order)
    col = col - y.astype(F32)
    col = jnp.where(col < 0.0, col + NY, col)
    shift_x = dest_x - x.astype(F32)
    shift_x = jnp.where(shift_x < 0.0, shift_x + NX, shift_x)
    shift_k = jnp.abs(dest_k - k.astype(F32))
    turn = shift_x * NK + shift_k
    group = order * NJ + turn
    at_group = one_if(fiota((GROUPS, count), 0) == group)
    at_owner = one_if(fiota((GROUPS * NY, count), 0) == group * NY + col)
    earlier = one_if(iota((count, count), 0) < iota((count, count), 1), BF16)
    rank = rsum(dot(at_group.astype(BF16), earlier) * at_group, 0)
    rank_owner = rsum(dot(at_owner.astype(BF16), earlier) * at_owner, 0)
    is_main = rank < float(MAIN)
    main_at = jnp.where(is_main, group * MAIN + rank, -1.0)
    spill_at = jnp.where(is_main, -8.0, group * MAIN + (rank - MAIN) * 4.0)
    assign[...] = at_group
    place[...] = col * (2.0 * CAP) + rank_owner

    value = col * float(ROWS) + turn * CAP + rank_owner + 1.0
    lane = fiota((128, count), 0)
    main_lane = jnp.where(is_main, turn * MAIN + rank, -8.0)
    spill_lane = jnp.where(is_main, -8.0, 64.0 + turn * MAIN + (rank - MAIN) * 4.0)
    hit = (lane == main_lane) | ((lane >= spill_lane) & (lane < spill_lane + 4.0))
    first = dot(at_group.astype(BF16), jnp.where(hit, value, 0.0).astype(BF16), ((1,), (1,)))
    hit = lane == value - 1.0
    high = jnp.floor((local + 1.0) * (1.0 / 16.0))
    low = local + 1.0 - high * 16.0
    second = 16.0 * dot(at_group.astype(BF16), jnp.where(hit, high, 0.0).astype(BF16), ((1,), (1,)))
    second += dot(at_group.astype(BF16), jnp.where(hit, low, 0.0).astype(BF16), ((1,), (1,)))
    both = jnp.concatenate([first, second], axis=1)
    for g in range(GROUPS):
        tag_out[g] = both[g : g + 1, :]
    tag_in[0] = tag_out[0]

    half = GROUPS // 2

    def pack(h):
        at = fiota((half * MAIN, count), 0) + float(h * half * MAIN)
        pick = one_if(at == main_at, BF16)
        for q in range(4):
            cols = slice(q * quarter, (q + 1) * quarter)
            packed = dot(pick, docs[:, cols]).astype(BF16)
            out[h * half : (h + 1) * half, :, cols] = packed.reshape(half, MAIN, quarter)
        spilled = jnp.zeros((half * MAIN, quarter), F32)
        for q in range(4):
            cols = slice(q * quarter, (q + 1) * quarter)
            spilled += dot(one_if(at == spill_at + float(q), BF16), docs[:, cols])
        out[h * half : (h + 1) * half, :, width:] = spilled.astype(BF16).reshape(half, MAIN, quarter)

    def send(ref_out, ref_in, sems, n, t, sign=1):
        px, pz, pk = peer(STEPS[n], t, sign)
        pltpu.make_async_remote_copy(
            src_ref=ref_out.at[n * NJ + t],
            dst_ref=ref_in.at[n * NJ + t],
            send_sem=sems[0],
            recv_sem=sems[1],
            device_id=(px, pz, pk, y),
            device_id_type=MESH,
        ).start()

    def send_group(ref_out, ref_in, sems, n, sign=1, first=0, last=NJ):
        def body(t, carry):
            send(ref_out, ref_in, sems, n, t, sign)
            return carry

        lax.fori_loop(max(first, 1 if n == 0 else 0), last, body, 0)

    def send_docs(n):
        odd = lax.rem(n, 2)
        dz = lax.rem(odd * ((n + 1) // 2) + (1 - odd) * (NZ - n // 2), NZ)

        def body(t, carry):
            px, pz, pk = peer(dz, t)
            pltpu.make_async_remote_copy(
                src_ref=out.at[n * NJ + t],
                dst_ref=inbox.at[n * NJ + t],
                send_sem=doc_send.at[n],
                recv_sem=doc_recv.at[n + (n // (NZ - 1)) * (t // (NJ // 2))],
                device_id=(px, pz, pk, y),
                device_id_type=MESH,
            ).start()
            return carry

        lax.fori_loop(1 if isinstance(n, int) and n == 0 else 0, NJ, body, 0)

    def send_tags(n):
        send_group(tag_out, tag_in, (tag_send, tag_recv.at[n]), n)

    def arrived(ref, sem):
        pltpu.make_async_copy(ref, ref, sem).wait()

    def y_send(dy, src, dst, send, recv):
        return pltpu.make_async_remote_copy(
            src_ref=src, dst_ref=dst, send_sem=send, recv_sem=recv,
            device_id=(x, z, k, lax.rem(y + dy, NY)), device_id_type=MESH,
        )

    load_docs.wait()
    pack(0)
    pl.semaphore_wait(barrier, NJ - 1 + NY - 1 + 2)
    ring_signal(0)
    send_tags(0)
    send_docs(0)
    ring_wait(0)
    ring_signal(1)
    for n in (1, 2):
        send_tags(n)
    for n in (1, 2):
        send_docs(n)
    inbox[0] = out[0]
    ring_wait(1)
    ring_signal(2)
    for n in (3, 4):
        send_tags(n)
    send_docs(3)
    pack(1)
    send_docs(4)
    ring_wait(2)
    ring_signal(3)
    for n in (5, 6):
        send_tags(n)
    ring_wait(3)
    send_tags(7)

    tot[...] = jnp.zeros_like(tot)
    best[...] = jnp.zeros_like(best)
    rowbest[...] = jnp.zeros_like(rowbest)

    def relay_tags(n, waited):
        arrived(tag_in.at[pl.ds(0, waited)], tag_recv.at[n])
        own = tag_in[n * NJ]
        for j in range(1, NJ):
            own += tag_in[n * NJ + j]
        own_out[n] = own
        for dy in range(1, NY):
            y_send(dy, own_out.at[n], own_in.at[dy, n], own_send, own_recv.at[n]).start()

    def relay(n, waited, sem, first=0, many=NJ):
        arrived(inbox.at[pl.ds(0, waited)], doc_recv.at[sem])
        marks = own_out[n]
        deep, tall = many * MAIN, many * CAP
        at = iota((NY * tall, deep), 0)
        target = ((at // tall) * ROWS + first * CAP + lax.rem(at, tall) + 1).astype(F32)
        pick = one_if(target == marks[:, first * MAIN : first * MAIN + deep], BF16)
        spill = target == marks[:, 64 + first * MAIN : 64 + first * MAIN + deep]
        phase = lax.rem(iota((NY * tall, deep), 1), 4)
        got = inbox[pl.ds(n * NJ + first, many)].reshape(deep, width + quarter)
        for q in range(4):
            cols = slice(q * quarter, (q + 1) * quarter)
            rows = dot(pick, got[:, cols])
            rows += dot(one_if(spill & (phase == q), BF16), got[:, width:])
            rows = rows.astype(BF16)
            block[n, first * CAP : first * CAP + tall, cols] = rows[:tall]
            for dy in range(1, NY):
                at_row = (dy - 1) * ROWS + first * CAP
                fwd[n, at_row : at_row + tall, cols] = rows[dy * tall : (dy + 1) * tall]
        for dy in range(1, NY):
            y_send(
                dy,
                fwd.at[n, pl.ds((dy - 1) * ROWS + first * CAP, tall)],
                block.at[n, pl.ds(dy * ROWS + first * CAP, tall)],
                fwd_send.at[n],
                fwd_recv.at[n],
            ).start()

    eye = iota((BLOCK, BLOCK), 0) == iota((BLOCK, BLOCK), 1)
    source = iota((1, 128), 1) // ROWS

    def owner_block(n, last=False):
        arrived(block.at[n, pl.ds(0, BLOCK - ROWS)], fwd_recv.at[n])
        mine = block[n]
        arrived(own_out.at[pl.ds(0, NY - 1)], own_recv.at[n])
        tag = own_out[n][:, 128:]
        for dy in range(1, NY):
            tag = jnp.where(source == dy, own_in[dy, n][:, 128:], tag)
        tags[pl.ds(n, 1), :] = tag
        live = tag > 0.0
        gram = dot(mine, mine, ((1,), (1,)))
        square = jnp.where(eye, gram, 0.0)
        scale = lax.rsqrt(rsum(square, 0) + 1.0)
        scale_col = lax.rsqrt(rsum(square, 1) + 1.0)
        tag_col = rsum(jnp.where(eye, jnp.broadcast_to(tag, (BLOCK, BLOCK)), 0.0), 1)
        rowscale[n] = jnp.broadcast_to(scale_col, (BLOCK, BLOCK))
        rowtag[n] = jnp.broadcast_to(tag_col, (BLOCK, BLOCK))
        pair = jnp.where((tag_col == tag) & live & jnp.logical_not(eye), gram, 0.0)
        top = rmax(pair * scale_col, 0)

        def meet(m, other, top):
            pair = jnp.where((rowtag[m] == tag) & live, other, 0.0)
            rowbest[m] = jnp.maximum(rowbest[m], pair * scale)
            return jnp.maximum(top, rmax(pair * rowscale[m], 0))

        if last:
            for begin, end in ((0, 4), (4, NZ - 1)):
                rows = (end - begin) * BLOCK
                others = dot(block[begin:end].reshape(rows, width), mine, ((1,), (1,)))
                for m in range(begin, end):
                    top = meet(m, others[(m - begin) * BLOCK : (m - begin + 1) * BLOCK], top)
        else:

            def earlier_block(m, top):
                return meet(m, dot(block[m], mine, ((1,), (1,))), top)

            top = lax.fori_loop(0, n, earlier_block, top)
        best[pl.ds(n, 1), :] = top * scale

        cross = dot(cents[...], mine, ((1,), (1,)))
        member = (fiota((table, BLOCK), 0) + 1.0) == tag
        similar = rsum(jnp.where(member, cross * qcol[...], 0.0), 0) * scale
        simil[pl.ds(n, 1), :] = similar
        tot[0] += one_if(member)
        tot[1] += jnp.where(member, similar, 0.0)
        tot[2] += jnp.where(member, similar * similar, 0.0)

    relay_tags(0, NJ - 1)
    relay(0, NJ - 1, 0)
    load_cents.wait()
    squares = jnp.zeros((table, 128), F32)
    for c in range(width // 128):
        part = cents[:, c * 128 : (c + 1) * 128].astype(F32)
        squares += part * part
    qcol[...] = lax.rsqrt(rsum(squares, 1) + 1.0)


    def main_step(i, carry):
        for n in (2 * i + 1, 2 * i + 2):
            relay_tags(n, NJ)
            relay(n, NJ, n)
        for n in (2 * i + 5, 2 * i + 6):

            @pl.when(n < NZ)
            def _():
                send_docs(n)

        @pl.when(i > 0)
        def _():
            owner_block(2 * i - 1)

        owner_block(2 * i)
        return carry

    lax.fori_loop(0, (NZ - 2) // 2, main_step, 0)
    relay_tags(NZ - 1, NJ)
    relay(NZ - 1, NJ // 2, NZ - 1, 0, NJ // 2)
    owner_block(NZ - 3)
    relay(NZ - 1, NJ // 2, NZ, NJ // 2, NJ // 2)
    owner_block(NZ - 2)
    owner_block(NZ - 1, last=True)

    counts = rsum(tot[0], 1)
    sums = rsum(tot[1], 1)
    squares = rsum(tot[2], 1)
    pos = iota((table, 128), 1)
    stacked = jnp.where(pos == 0, counts, jnp.where(pos == 1, sums, jnp.where(pos == 2, squares, 0.0)))
    stats_ref[...] = stacked.T[:3]
    floor = jnp.maximum(counts, 1.0)
    mean = sums / floor
    spread = jnp.sqrt(jnp.maximum(squares / floor - mean * mean, 0.0) + 1.0 / width)

    def scores(n, carry):
        tag = tags[pl.ds(n, 1), :]
        member = (fiota((table, BLOCK), 0) + 1.0) == tag
        mean_at = rsum(jnp.where(member, mean, 0.0), 0)
        spread_at = rsum(jnp.where(member, spread, 0.0), 0)
        gap = (mean_at - simil[pl.ds(n, 1), :]) / jnp.where(tag > 0.0, spread_at, 1.0)
        score[0, pl.ds(n, 1), :] = jnp.where(tag > 0.0, gap, 0.0)
        rows = rmax((rowbest[n] * rowscale[n]).T, 0)
        score[1, pl.ds(n, 1), :] = math.sqrt(width) * jnp.maximum(best[pl.ds(n, 1), :], rows)
        return carry

    lax.fori_loop(0, NZ, scores, 0)
    for dy in range(1, NY):
        y_send(NY - dy, score, score_in.at[dy], score_send, score_recv).start()
    score_in[0] = score[...]

    arrived(score_in.at[pl.ds(1, NY - 1)], score_recv)
    lanes = iota((GROUPS, 128), 1)
    mine = lax.rem(lanes, ROWS) // CAP == lax.rem(iota((GROUPS, 128), 0), NJ)
    from_lane, to_lane = iota((128, 128), 0), iota((128, 128), 1)
    laid = jnp.zeros((GROUPS, 128), F32)
    for s in range(2):
        held = jnp.zeros((NZ, 128), F32)
        for dy in range(NY):
            held = jnp.where(iota((NZ, 128), 1) // ROWS == dy, score_in[dy, s], held)
        held = jnp.broadcast_to(held[:, None, :], (NZ, NJ, 128)).reshape(GROUPS, 128)
        move = one_if(to_lane == (from_lane // ROWS) * (2 * CAP) + s * CAP + lax.rem(from_lane, CAP))
        laid += dot(jnp.where(mine, held, 0.0), move, precision=HIGHEST)
    for g in range(GROUPS):
        reply[g] = laid[g : g + 1, :]

    for n in reversed(range(NZ)):
        send_group(reply, reply_in, (reply_send, reply_recv), n, sign=-1)
    reply_in[0] = reply[0]

    for n, dz in enumerate(STEPS):
        arrived(inbox.at[pl.ds(0, NJ - 1 if dz == 0 else NJ)], doc_send.at[n])
        arrived(fwd.at[n], fwd_send.at[n])
    arrived(tag_out.at[pl.ds(0, GROUPS - 1)], tag_send)
    for dy in range(1, NY):
        arrived(own_in.at[dy], own_send)
    arrived(score_in.at[pl.ds(1, NY - 1)], score_send)
    arrived(reply.at[pl.ds(0, GROUPS - 1)], reply_send)
    arrived(reply_in.at[pl.ds(0, GROUPS - 1)], reply_recv)


def unpack(reply_ref, assign, place, stats_ref, proto_ref, red_ref, totals_ref):
    count = assign.shape[1]
    home = jnp.concatenate(
        [reply_ref[...].reshape(GROUPS, 128), jnp.zeros((128 - GROUPS, 128), F32)], axis=0
    ).T
    picked = dot(home[: NY * 2 * CAP, :GROUPS], assign[...], precision=HIGHEST)
    at = fiota((NY * 2 * CAP, count), 0)
    proto_ref[...] = rsum(jnp.where(at == place[...], picked, 0.0), 0)
    red_ref[...] = rsum(jnp.where(at == place[...] + CAP, picked, 0.0), 0)
    totals_ref[...] = stats_ref[...]


def local(documents, assigned, centroids, owner_slot):
    count, width = documents.shape
    table = centroids.shape[0]
    wide = width + width // 4
    dma = pltpu.SemaphoreType.DMA
    outs = (
        jax.ShapeDtypeStruct((1, count), F32),
        jax.ShapeDtypeStruct((1, count), F32),
        jax.ShapeDtypeStruct((3, table), F32),
    )
    vmem = pl.BlockSpec(memory_space=pltpu.VMEM)
    parts = pl.pallas_call(
        kernel,
        out_shape=(
            jax.ShapeDtypeStruct((GROUPS, 1, 128), F32),
            jax.ShapeDtypeStruct((GROUPS, count), F32),
            jax.ShapeDtypeStruct((1, count), F32),
            jax.ShapeDtypeStruct((3, table), F32),
        ),
        in_specs=[pl.BlockSpec(memory_space=pl.ANY)] * 4,
        out_specs=(vmem,) * 4,
        scratch_shapes=[
            pltpu.VMEM((1, count), jnp.int32),
            pltpu.VMEM((owner_slot.shape[0] // 128, 128), jnp.int32),
            pltpu.VMEM((count, width), BF16),
            pltpu.VMEM((table, width), BF16),
            pltpu.VMEM((GROUPS, MAIN, wide), BF16),
            pltpu.VMEM((GROUPS, MAIN, wide), BF16),
            pltpu.VMEM((NZ, BLOCK - ROWS, width), BF16),
            pltpu.VMEM((NZ, BLOCK, width), BF16),
            pltpu.VMEM((GROUPS, 1, 256), F32),
            pltpu.VMEM((GROUPS, 1, 256), F32),
            pltpu.VMEM((NZ, 1, 256), F32),
            pltpu.VMEM((NY, NZ, 1, 256), F32),
            pltpu.VMEM((table, 1), F32),
            pltpu.VMEM((NZ, BLOCK), F32),
            pltpu.VMEM((NZ, BLOCK, BLOCK), F32),
            pltpu.VMEM((NZ, BLOCK, BLOCK), F32),
            pltpu.VMEM((NZ, BLOCK), F32),
            pltpu.VMEM((NZ, BLOCK), F32),
            pltpu.VMEM((NZ, BLOCK, BLOCK), F32),
            pltpu.VMEM((3, table, BLOCK), F32),
            pltpu.VMEM((2, NZ, BLOCK), F32),
            pltpu.VMEM((NY, 2, NZ, BLOCK), F32),
            pltpu.VMEM((GROUPS, 1, 128), F32),
            pltpu.SemaphoreType.REGULAR((NZ // 2, 2)),
            dma((4,)),
            dma((NZ,)), dma((NZ + 1,)),
            dma, dma((NZ,)),
            dma, dma((NZ,)),
            dma((NZ,)), dma((NZ,)),
            dma, dma,
            dma, dma,
        ],
        compiler_params=pltpu.CompilerParams(
            collective_id=0, has_side_effects=True, vmem_limit_bytes=56 * 1024 * 1024
        ),
        name="route_and_score",
    )(assigned.reshape(1, count), owner_slot.reshape(-1, 128), documents, centroids)
    proto, red, stats = pl.pallas_call(
        unpack,
        out_shape=outs,
        in_specs=[vmem] * 4,
        out_specs=(vmem,) * 3,
        name="unpack",
    )(*parts)
    return proto.reshape(count), red.reshape(count), stats


def solution(mesh):
    split = Mesh(mesh.devices.reshape(NX, NZ, NK, NY), AXES)
    placed = (P(AXES, None), P(AXES), P(AXES, None), P())
    return jax.shard_map(
        local,
        mesh=split,
        in_specs=placed,
        out_specs=(P(AXES), P(AXES), P(None, AXES)),
        check_vma=False,
    )
```

```python
import math

import jax
import jax.numpy as jnp
from jax import lax
from jax.experimental import pallas as pl
from jax.experimental.pallas import tpu as pltpu
from jax.sharding import Mesh
from jax.sharding import PartitionSpec as P

AXES = ("dp_0", "dp_1", "dp_2", "cent")
MESH = pl.DeviceIdType.MESH
F32 = jnp.float32
BF16 = jnp.bfloat16
HIGHEST = lax.Precision.HIGHEST

NX, NZ, NK, NY = 4, 8, 2, 4
NJ = NX * NK
GROUPS = NZ * NJ
MAIN, SPILL, CAP = 8, 2, 4
STEPS = tuple((n + 1) // 2 if n % 2 else -(n // 2) % NZ for n in range(NZ))
ROWS = NJ * CAP
PLANE_FIRST, PLANE_THEN = (1, 2, 3), (4, 0, 5, 6, 7)
BLOCK = NY * ROWS


def dot(a, b, dims=((1,), (0,)), precision=None):
    return lax.dot_general(a, b, (dims, ((), ())), precision=precision, preferred_element_type=F32)


def iota(shape, dim):
    return lax.broadcasted_iota(jnp.int32, shape, dim)


def fiota(shape, dim):
    return iota(shape, dim).astype(F32)


def rsum(value, axis):
    return jnp.sum(value, axis=axis, keepdims=True)


def rmax(value, axis):
    return jnp.max(value, axis=axis, keepdims=True)


def one_if(mask, dtype=F32):
    return jnp.where(mask, 1.0, 0.0).astype(dtype)


def kernel(
    assigned_hbm, slots_hbm, docs_hbm, cents_hbm,
    reply_in, group_ref, place, stats_ref,
    assigned, slots, docs, cents, out, mid, inbox, fwd, block,
    tag_out, tag_in, own_out, own_in,
    qcol, tags, rowscale, rowtag, simil, best, rowbest, tot,
    score, score_in, reply,
    ring, load_sem, doc_send, hop_send, mid_recv, doc_recv, tag_send, tag_recv, own_send, own_recv,
    fwd_send, fwd_recv, score_send, score_recv, reply_send, reply_recv,
):
    x, z, k, y = (lax.axis_index(a) for a in AXES)
    count, width = docs.shape
    table = cents.shape[0]
    quarter = width // 4

    load_assigned = pltpu.make_async_copy(assigned_hbm, assigned, load_sem.at[2])
    load_slots = pltpu.make_async_copy(slots_hbm, slots, load_sem.at[3])
    load_docs = pltpu.make_async_copy(docs_hbm, docs, load_sem.at[0])
    load_cents = pltpu.make_async_copy(cents_hbm, cents, load_sem.at[1])
    load_assigned.start()
    load_slots.start()
    load_docs.start()
    load_cents.start()

    def peer(dz, t, sign=1):
        px = lax.rem(x + NX + sign * (t // NK), NX)
        pk = lax.rem(k + NK + sign * lax.rem(t, NK), NK)
        pz = lax.rem(z + NZ + sign * dz, NZ)
        return px, pz, pk

    barrier = pltpu.get_barrier_semaphore()

    def hello(sem, px, pz, pk, py):
        pl.semaphore_signal(sem, inc=1, device_id=(px, pz, pk, py), device_id_type=MESH)

    above, below = lax.rem(z + 1, NZ), lax.rem(z + NZ - 1, NZ)
    hello(barrier, x, above, k, y)
    hello(barrier, x, below, k, y)
    for t in range(1, NJ):
        px, pz, pk = peer(0, t)
        hello(barrier, px, pz, pk, y)
    for dy in range(1, NY):
        hello(barrier, x, z, k, lax.rem(y + dy, NY))

    def ring_signal(r):
        hello(ring.at[r, 0], x, above, k, y)
        hello(ring.at[r, 1], x, below, k, y)

    def ring_wait(r):
        pl.semaphore_wait(ring.at[r, 0], 1)
        pl.semaphore_wait(ring.at[r, 1], 1)

    load_assigned.wait()
    load_slots.wait()
    number = assigned[...].astype(F32)
    at_row = jnp.floor(number * (1.0 / 128.0))
    at_lane = number - at_row * 128.0
    held = slots.shape[0]
    turned = jnp.concatenate(
        [slots[r * 128 : (r + 1) * 128, :].astype(F32).T for r in range(held // 128)], axis=1
    )
    top = jnp.floor(turned * (1.0 / 4096.0))
    turned -= top * 4096.0
    middle = jnp.floor(turned * (1.0 / 64.0))
    turned -= middle * 64.0
    digits = jnp.concatenate([top, middle, turned], axis=0).astype(BF16)
    digits = dot(digits, one_if(fiota((held, count), 0) == at_row, BF16))
    slot = digits[:128] * 4096.0 + digits[128:256] * 64.0 + digits[256:]
    slot = rsum(jnp.where(fiota((128, count), 0) == at_lane, slot, 0.0), 0)

    owner = jnp.floor((slot + 0.5) * (1.0 / table))
    local = slot - owner * table
    row = jnp.floor(owner * (1.0 / NY))
    col = owner - row * NY
    dest_x = jnp.floor(row * (1.0 / (NZ * NK)))
    rest = row - dest_x * (NZ * NK)
    dest_z = jnp.floor(rest * (1.0 / NK))
    dest_k = rest - dest_z * NK
    step = dest_z - z.astype(F32)
    step = jnp.where(step < 0.0, step + NZ, step)
    order = jnp.zeros_like(step)
    for n, dz in enumerate(STEPS):
        order = jnp.where(step == float(dz), float(n), order)
    col = col - y.astype(F32)
    col = jnp.where(col < 0.0, col + NY, col)
    shift_x = dest_x - x.astype(F32)
    shift_x = jnp.where(shift_x < 0.0, shift_x + NX, shift_x)
    shift_k = jnp.abs(dest_k - k.astype(F32))
    turn = shift_x * NK + shift_k
    group = order * NJ + turn
    at_group = one_if(fiota((GROUPS, count), 0) == group)
    at_owner = one_if(fiota((GROUPS * NY, count), 0) == group * NY + col)
    earlier = one_if(iota((count, count), 0) < iota((count, count), 1), BF16)
    rank = rsum(dot(at_group.astype(BF16), earlier) * at_group, 0)
    rank_owner = rsum(dot(at_owner.astype(BF16), earlier) * at_owner, 0)
    is_main = rank < float(MAIN)
    main_at = jnp.where(is_main, group * MAIN + rank, -1.0)
    spill_at = jnp.where(is_main, -8.0, group * MAIN + (rank - MAIN) * 4.0)
    group_ref[...] = group
    place[...] = col * (2.0 * CAP) + rank_owner

    value = col * float(ROWS) + turn * CAP + rank_owner + 1.0
    lane = fiota((128, count), 0)
    main_lane = jnp.where(is_main, turn * MAIN + rank, -8.0)
    spill_lane = jnp.where(is_main, -8.0, 64.0 + turn * MAIN + (rank - MAIN) * 4.0)
    hit = (lane == main_lane) | ((lane >= spill_lane) & (lane < spill_lane + 4.0))
    first = dot(at_group.astype(BF16), jnp.where(hit, value, 0.0).astype(BF16), ((1,), (1,)))
    hit = lane == value - 1.0
    high = jnp.floor((local + 1.0) * (1.0 / 16.0))
    low = local + 1.0 - high * 16.0
    second = 16.0 * dot(at_group.astype(BF16), jnp.where(hit, high, 0.0).astype(BF16), ((1,), (1,)))
    second += dot(at_group.astype(BF16), jnp.where(hit, low, 0.0).astype(BF16), ((1,), (1,)))
    both = jnp.concatenate([first, second], axis=1)
    for g in range(GROUPS):
        tag_out[g] = both[g : g + 1, :]
    tag_in[0] = tag_out[0]

    half = GROUPS // 2

    def pack(h):
        at = fiota((half * MAIN, count), 0) + float(h * half * MAIN)
        pick = one_if(at == main_at, BF16)
        for q in range(4):
            cols = slice(q * quarter, (q + 1) * quarter)
            packed = dot(pick, docs[:, cols]).astype(BF16)
            out[h * half : (h + 1) * half, :, cols] = packed.reshape(half, MAIN, quarter)
        spilled = jnp.zeros((half * MAIN, quarter), F32)
        for q in range(4):
            cols = slice(q * quarter, (q + 1) * quarter)
            spilled += dot(one_if(at == spill_at + float(q), BF16), docs[:, cols])
        out[h * half : (h + 1) * half, :, width:] = spilled.astype(BF16).reshape(half, MAIN, quarter)

    def send(ref_out, ref_in, sems, n, t, sign=1):
        px, pz, pk = peer(STEPS[n], t, sign)
        pltpu.make_async_remote_copy(
            src_ref=ref_out.at[n * NJ + t],
            dst_ref=ref_in.at[n * NJ + t],
            send_sem=sems[0],
            recv_sem=sems[1],
            device_id=(px, pz, pk, y),
            device_id_type=MESH,
        ).start()

    def send_group(ref_out, ref_in, sems, n, sign=1, first=0, last=NJ):
        def body(t, carry):
            send(ref_out, ref_in, sems, n, t, sign)
            return carry

        lax.fori_loop(max(first, 1 if n == 0 else 0), last, body, 0)

    def plane_send(n):
        ref_in, sems = (mid, (hop_send, mid_recv.at[n])) if n else (inbox, (doc_send.at[0], doc_recv.at[0]))

        def body(t, carry):
            px, pz, pk = peer(0, t)
            pltpu.make_async_remote_copy(
                src_ref=out.at[n * NJ + t],
                dst_ref=ref_in.at[n * NJ + t],
                send_sem=sems[0],
                recv_sem=sems[1],
                device_id=(px, pz, pk, y),
                device_id_type=MESH,
            ).start()
            return carry

        lax.fori_loop(1, NJ, body, 0)

    def z_send(n, ref_out, first, many):
        odd = lax.rem(n, 2)
        dz = lax.rem(odd * ((n + 1) // 2) + (1 - odd) * (NZ - n // 2), NZ)
        rows = pl.ds(n * NJ + first, many)
        pltpu.make_async_remote_copy(
            src_ref=ref_out.at[rows],
            dst_ref=inbox.at[rows],
            send_sem=doc_send.at[n],
            recv_sem=doc_recv.at[n + (n // (NZ - 1)) * (first // (NJ // 2))],
            device_id=(x, lax.rem(z + dz, NZ), k, y),
            device_id_type=MESH,
        ).start()

    def z_forward(n):
        arrived(mid.at[pl.ds(0, NJ - 1)], mid_recv.at[n])
        z_send(n, mid, 1, NJ // 2 - 1)
        z_send(n, mid, NJ // 2, NJ // 2)

    def send_tags(n):
        send_group(tag_out, tag_in, (tag_send, tag_recv.at[n]), n)

    def arrived(ref, sem):
        pltpu.make_async_copy(ref, ref, sem).wait()

    def y_send(dy, src, dst, send, recv):
        return pltpu.make_async_remote_copy(
            src_ref=src, dst_ref=dst, send_sem=send, recv_sem=recv,
            device_id=(x, z, k, lax.rem(y + dy, NY)), device_id_type=MESH,
        )

    load_docs.wait()
    pack(0)
    pl.semaphore_wait(barrier, NJ - 1 + NY - 1 + 2)
    ring_signal(0)
    send_tags(0)
    for n in PLANE_FIRST:
        plane_send(n)
    ring_wait(0)
    ring_signal(1)
    for n in (1, 2):
        send_tags(n)
        z_send(n, out, 0, 1)
    inbox[0] = out[0]
    pack(1)
    ring_wait(1)
    ring_signal(2)
    for n in (3, 4):
        send_tags(n)
        z_send(n, out, 0, 1)
    for n in PLANE_THEN:
        plane_send(n)
    ring_wait(2)
    ring_signal(3)
    for n in (5, 6):
        send_tags(n)
        z_send(n, out, 0, 1)
    ring_wait(3)
    send_tags(7)
    z_send(7, out, 0, 1)
    for n in (1, 2, 3, 4):
        z_forward(n)

    tot[...] = jnp.zeros_like(tot)
    best[...] = jnp.zeros_like(best)
    rowbest[...] = jnp.zeros_like(rowbest)

    def relay_tags(n, waited):
        arrived(tag_in.at[pl.ds(0, waited)], tag_recv.at[n])
        own = tag_in[n * NJ]
        for j in range(1, NJ):
            own += tag_in[n * NJ + j]
        own_out[n] = own
        for dy in range(1, NY):
            y_send(dy, own_out.at[n], own_in.at[dy, n], own_send, own_recv.at[n]).start()

    def relay(n, waited, sem, first=0, many=NJ):
        arrived(inbox.at[pl.ds(0, waited)], doc_recv.at[sem])
        marks = own_out[n]
        deep, tall = many * MAIN, many * CAP
        at = iota((NY * tall, deep), 0)
        target = ((at // tall) * ROWS + first * CAP + lax.rem(at, tall) + 1).astype(F32)
        pick = one_if(target == marks[:, first * MAIN : first * MAIN + deep], BF16)
        spill = target == marks[:, 64 + first * MAIN : 64 + first * MAIN + deep]
        phase = lax.rem(iota((NY * tall, deep), 1), 4)
        got = inbox[pl.ds(n * NJ + first, many)].reshape(deep, width + quarter)
        for q in range(4):
            cols = slice(q * quarter, (q + 1) * quarter)
            rows = dot(pick, got[:, cols])
            rows += dot(one_if(spill & (phase == q), BF16), got[:, width:])
            rows = rows.astype(BF16)
            block[n, first * CAP : first * CAP + tall, cols] = rows[:tall]
            for dy in range(1, NY):
                at_row = (dy - 1) * ROWS + first * CAP
                fwd[n, at_row : at_row + tall, cols] = rows[dy * tall : (dy + 1) * tall]
        for dy in range(1, NY):
            y_send(
                dy,
                fwd.at[n, pl.ds((dy - 1) * ROWS + first * CAP, tall)],
                block.at[n, pl.ds(dy * ROWS + first * CAP, tall)],
                fwd_send.at[n],
                fwd_recv.at[n],
            ).start()

    eye = iota((BLOCK, BLOCK), 0) == iota((BLOCK, BLOCK), 1)
    source = iota((1, 128), 1) // ROWS

    def owner_block(n, last=False):
        arrived(block.at[n, pl.ds(0, BLOCK - ROWS)], fwd_recv.at[n])
        mine = block[n]
        arrived(own_out.at[pl.ds(0, NY - 1)], own_recv.at[n])
        tag = own_out[n][:, 128:]
        for dy in range(1, NY):
            tag = jnp.where(source == dy, own_in[dy, n][:, 128:], tag)
        tags[pl.ds(n, 1), :] = tag
        live = tag > 0.0
        gram = dot(mine, mine, ((1,), (1,)))
        square = jnp.where(eye, gram, 0.0)
        scale = lax.rsqrt(rsum(square, 0) + 1.0)
        scale_col = lax.rsqrt(rsum(square, 1) + 1.0)
        tag_col = rsum(jnp.where(eye, jnp.broadcast_to(tag, (BLOCK, BLOCK)), 0.0), 1)
        rowscale[n] = jnp.broadcast_to(scale_col, (BLOCK, BLOCK))
        rowtag[n] = jnp.broadcast_to(tag_col, (BLOCK, BLOCK))
        pair = jnp.where((tag_col == tag) & live & jnp.logical_not(eye), gram, 0.0)
        top = rmax(pair * scale_col, 0)

        def meet(m, other, top):
            pair = jnp.where((rowtag[m] == tag) & live, other, 0.0)
            rowbest[m] = jnp.maximum(rowbest[m], pair * scale)
            return jnp.maximum(top, rmax(pair * rowscale[m], 0))

        if last:
            for begin, end in ((0, 4), (4, NZ - 1)):
                rows = (end - begin) * BLOCK
                others = dot(block[begin:end].reshape(rows, width), mine, ((1,), (1,)))
                for m in range(begin, end):
                    top = meet(m, others[(m - begin) * BLOCK : (m - begin + 1) * BLOCK], top)
        else:

            def earlier_block(m, top):
                return meet(m, dot(block[m], mine, ((1,), (1,))), top)

            top = lax.fori_loop(0, n, earlier_block, top)
        best[pl.ds(n, 1), :] = top * scale

        cross = dot(cents[...], mine, ((1,), (1,)))
        member = (fiota((table, BLOCK), 0) + 1.0) == tag
        similar = rsum(jnp.where(member, cross * qcol[...], 0.0), 0) * scale
        simil[pl.ds(n, 1), :] = similar
        tot[0] += one_if(member)
        tot[1] += jnp.where(member, similar, 0.0)
        tot[2] += jnp.where(member, similar * similar, 0.0)

    relay_tags(0, NJ - 1)
    relay(0, NJ - 1, 0)
    load_cents.wait()
    squares = jnp.zeros((table, 128), F32)
    for c in range(width // 128):
        part = cents[:, c * 128 : (c + 1) * 128].astype(F32)
        squares += part * part
    qcol[...] = lax.rsqrt(rsum(squares, 1) + 1.0)


    def main_step(i, carry):
        for n in (2 * i + 1, 2 * i + 2):
            relay_tags(n, NJ)
            relay(n, NJ, n)
        for n in (2 * i + 5, 2 * i + 6):

            @pl.when(n < NZ)
            def _():
                z_forward(n)

        @pl.when(i > 0)
        def _():
            owner_block(2 * i - 1)

        owner_block(2 * i)
        return carry

    lax.fori_loop(0, (NZ - 2) // 2, main_step, 0)
    relay_tags(NZ - 1, NJ)
    relay(NZ - 1, NJ // 2, NZ - 1, 0, NJ // 2)
    owner_block(NZ - 3)
    relay(NZ - 1, NJ // 2, NZ, NJ // 2, NJ // 2)
    owner_block(NZ - 2)
    owner_block(NZ - 1, last=True)

    counts = rsum(tot[0], 1)
    sums = rsum(tot[1], 1)
    squares = rsum(tot[2], 1)
    pos = iota((table, 128), 1)
    stacked = jnp.where(pos == 0, counts, jnp.where(pos == 1, sums, jnp.where(pos == 2, squares, 0.0)))
    stats_ref[...] = stacked.T[:3]
    floor = jnp.maximum(counts, 1.0)
    mean = sums / floor
    spread = jnp.sqrt(jnp.maximum(squares / floor - mean * mean, 0.0) + 1.0 / width)

    def scores(n, carry):
        tag = tags[pl.ds(n, 1), :]
        member = (fiota((table, BLOCK), 0) + 1.0) == tag
        mean_at = rsum(jnp.where(member, mean, 0.0), 0)
        spread_at = rsum(jnp.where(member, spread, 0.0), 0)
        gap = (mean_at - simil[pl.ds(n, 1), :]) / jnp.where(tag > 0.0, spread_at, 1.0)
        score[0, pl.ds(n, 1), :] = jnp.where(tag > 0.0, gap, 0.0)
        rows = rmax((rowbest[n] * rowscale[n]).T, 0)
        score[1, pl.ds(n, 1), :] = math.sqrt(width) * jnp.maximum(best[pl.ds(n, 1), :], rows)
        return carry

    lax.fori_loop(0, NZ, scores, 0)
    for dy in range(1, NY):
        y_send(NY - dy, score, score_in.at[dy], score_send, score_recv).start()
    score_in[0] = score[...]

    arrived(score_in.at[pl.ds(1, NY - 1)], score_recv)
    lanes = iota((GROUPS, 128), 1)
    mine = lax.rem(lanes, ROWS) // CAP == lax.rem(iota((GROUPS, 128), 0), NJ)
    from_lane, to_lane = iota((128, 128), 0), iota((128, 128), 1)
    laid = jnp.zeros((GROUPS, 128), F32)
    for s in range(2):
        held = jnp.zeros((NZ, 128), F32)
        for dy in range(NY):
            held = jnp.where(iota((NZ, 128), 1) // ROWS == dy, score_in[dy, s], held)
        held = jnp.broadcast_to(held[:, None, :], (NZ, NJ, 128)).reshape(GROUPS, 128)
        move = one_if(to_lane == (from_lane // ROWS) * (2 * CAP) + s * CAP + lax.rem(from_lane, CAP))
        laid += dot(jnp.where(mine, held, 0.0), move, precision=HIGHEST)
    for g in range(GROUPS):
        reply[g] = laid[g : g + 1, :]

    for n in reversed(range(NZ)):
        send_group(reply, reply_in, (reply_send, reply_recv), n, sign=-1)
    reply_in[0] = reply[0]

    for n, dz in enumerate(STEPS):
        arrived(inbox.at[pl.ds(0, NJ - 1 if dz == 0 else NJ)], doc_send.at[n])
        arrived(fwd.at[n], fwd_send.at[n])
    arrived(tag_out.at[pl.ds(0, GROUPS - 1)], tag_send)
    arrived(inbox.at[pl.ds(0, (NZ - 1) * (NJ - 1))], hop_send)
    for dy in range(1, NY):
        arrived(own_in.at[dy], own_send)
    arrived(score_in.at[pl.ds(1, NY - 1)], score_send)
    arrived(reply.at[pl.ds(0, GROUPS - 1)], reply_send)
    arrived(reply_in.at[pl.ds(0, GROUPS - 1)], reply_recv)


def unpack(reply_ref, group_ref, place, stats_ref, proto_ref, red_ref, totals_ref):
    count = group_ref.shape[1]
    assign = one_if(fiota((GROUPS, count), 0) == group_ref[...])
    home = jnp.concatenate(
        [reply_ref[...].reshape(GROUPS, 128), jnp.zeros((128 - GROUPS, 128), F32)], axis=0
    ).T
    picked = dot(home[: NY * 2 * CAP, :GROUPS], assign, precision=HIGHEST)
    at = fiota((NY * 2 * CAP, count), 0)
    proto_ref[...] = rsum(jnp.where(at == place[...], picked, 0.0), 0)
    red_ref[...] = rsum(jnp.where(at == place[...] + CAP, picked, 0.0), 0)
    totals_ref[...] = stats_ref[...]


def local(documents, assigned, centroids, owner_slot):
    count, width = documents.shape
    table = centroids.shape[0]
    wide = width + width // 4
    dma = pltpu.SemaphoreType.DMA
    outs = (
        jax.ShapeDtypeStruct((1, count), F32),
        jax.ShapeDtypeStruct((1, count), F32),
        jax.ShapeDtypeStruct((3, table), F32),
    )
    vmem = pl.BlockSpec(memory_space=pltpu.VMEM)
    parts = pl.pallas_call(
        kernel,
        out_shape=(
            jax.ShapeDtypeStruct((GROUPS, 1, 128), F32),
            jax.ShapeDtypeStruct((1, count), F32),
            jax.ShapeDtypeStruct((1, count), F32),
            jax.ShapeDtypeStruct((3, table), F32),
        ),
        in_specs=[pl.BlockSpec(memory_space=pl.ANY)] * 4,
        out_specs=(vmem,) * 4,
        scratch_shapes=[
            pltpu.VMEM((1, count), jnp.int32),
            pltpu.VMEM((owner_slot.shape[0] // 128, 128), jnp.int32),
            pltpu.VMEM((count, width), BF16),
            pltpu.VMEM((table, width), BF16),
            pltpu.VMEM((GROUPS, MAIN, wide), BF16),
            pltpu.VMEM((GROUPS, MAIN, wide), BF16),
            pltpu.VMEM((GROUPS, MAIN, wide), BF16),
            pltpu.VMEM((NZ, BLOCK - ROWS, width), BF16),
            pltpu.VMEM((NZ, BLOCK, width), BF16),
            pltpu.VMEM((GROUPS, 1, 256), F32),
            pltpu.VMEM((GROUPS, 1, 256), F32),
            pltpu.VMEM((NZ, 1, 256), F32),
            pltpu.VMEM((NY, NZ, 1, 256), F32),
            pltpu.VMEM((table, 1), F32),
            pltpu.VMEM((NZ, BLOCK), F32),
            pltpu.VMEM((NZ, BLOCK, BLOCK), F32),
            pltpu.VMEM((NZ, BLOCK, BLOCK), F32),
            pltpu.VMEM((NZ, BLOCK), F32),
            pltpu.VMEM((NZ, BLOCK), F32),
            pltpu.VMEM((NZ, BLOCK, BLOCK), F32),
            pltpu.VMEM((3, table, BLOCK), F32),
            pltpu.VMEM((2, NZ, BLOCK), F32),
            pltpu.VMEM((NY, 2, NZ, BLOCK), F32),
            pltpu.VMEM((GROUPS, 1, 128), F32),
            pltpu.SemaphoreType.REGULAR((NZ // 2, 2)),
            dma((4,)),
            dma((NZ,)), dma, dma((NZ,)), dma((NZ + 1,)),
            dma, dma((NZ,)),
            dma, dma((NZ,)),
            dma((NZ,)), dma((NZ,)),
            dma, dma,
            dma, dma,
        ],
        compiler_params=pltpu.CompilerParams(
            collective_id=0, has_side_effects=True, vmem_limit_bytes=56 * 1024 * 1024
        ),
        name="route_and_score",
    )(assigned.reshape(1, count), owner_slot.reshape(-1, 128), documents, centroids)
    proto, red, stats = pl.pallas_call(
        unpack,
        out_shape=outs,
        in_specs=[vmem] * 4,
        out_specs=(vmem,) * 3,
        name="unpack",
    )(*parts)
    return proto.reshape(count), red.reshape(count), stats


def solution(mesh):
    split = Mesh(mesh.devices.reshape(NX, NZ, NK, NY), AXES)
    placed = (P(AXES, None), P(AXES), P(AXES, None), P())
    return jax.shard_map(
        local,
        mesh=split,
        in_specs=placed,
        out_specs=(P(AXES), P(AXES), P(None, AXES)),
        check_vma=False,
    )
```

```python
import math

import jax
import jax.numpy as jnp
from jax import lax
from jax.experimental import pallas as pl
from jax.experimental.pallas import tpu as pltpu
from jax.sharding import Mesh
from jax.sharding import PartitionSpec as P

AXES = ("dp_0", "dp_1", "dp_2", "cent")
MESH = pl.DeviceIdType.MESH
F32 = jnp.float32
BF16 = jnp.bfloat16
HIGHEST = lax.Precision.HIGHEST

NX, NZ, NK, NY = 4, 8, 2, 4
NJ = NX * NK
GROUPS = NZ * NJ
MAIN, SPILL, CAP = 8, 2, 4
STEPS = tuple((n + 1) // 2 if n % 2 else -(n // 2) % NZ for n in range(NZ))
ROWS = NJ * CAP
PLANE_FIRST, PLANE_THEN = (1, 2, 3), (4, 0, 5, 6, 7)
BLOCK = NY * ROWS


def dot(a, b, dims=((1,), (0,)), precision=None):
    return lax.dot_general(a, b, (dims, ((), ())), precision=precision, preferred_element_type=F32)


def iota(shape, dim):
    return lax.broadcasted_iota(jnp.int32, shape, dim)


def fiota(shape, dim):
    return iota(shape, dim).astype(F32)


def rsum(value, axis):
    return jnp.sum(value, axis=axis, keepdims=True)


def rmax(value, axis):
    return jnp.max(value, axis=axis, keepdims=True)


def one_if(mask, dtype=F32):
    return jnp.where(mask, 1.0, 0.0).astype(dtype)


def kernel(
    assigned_hbm, slots_hbm, docs_hbm, cents_hbm,
    reply_in, group_ref, place, stats_ref,
    assigned, slots, docs, cents, out, mid, inbox, fwd, block,
    tag_out, tag_in, own_out, own_in,
    qcol, tags, rowscale, rowtag, simil, best, rowbest, tot,
    score, score_in, reply,
    ring, load_sem, doc_send, hop_send, mid_recv, doc_recv, tag_send, tag_recv, own_send, own_recv,
    fwd_send, fwd_recv, score_send, score_recv, reply_send, reply_recv,
):
    x, z, k, y = (lax.axis_index(a) for a in AXES)
    count, width = docs.shape
    table = cents.shape[0]
    quarter = width // 4

    load_assigned = pltpu.make_async_copy(assigned_hbm, assigned, load_sem.at[2])
    load_slots = pltpu.make_async_copy(slots_hbm, slots, load_sem.at[3])
    load_docs = pltpu.make_async_copy(docs_hbm, docs, load_sem.at[0])
    load_cents = pltpu.make_async_copy(cents_hbm, cents, load_sem.at[1])
    load_assigned.start()
    load_slots.start()
    load_docs.start()
    load_cents.start()

    def peer(dz, t, sign=1):
        px = lax.rem(x + NX + sign * (t // NK), NX)
        pk = lax.rem(k + NK + sign * lax.rem(t, NK), NK)
        pz = lax.rem(z + NZ + sign * dz, NZ)
        return px, pz, pk

    barrier = pltpu.get_barrier_semaphore()

    def hello(sem, px, pz, pk, py):
        pl.semaphore_signal(sem, inc=1, device_id=(px, pz, pk, py), device_id_type=MESH)

    above, below = lax.rem(z + 1, NZ), lax.rem(z + NZ - 1, NZ)
    hello(barrier, x, above, k, y)
    hello(barrier, x, below, k, y)
    for t in range(1, NJ):
        px, pz, pk = peer(0, t)
        hello(barrier, px, pz, pk, y)
    for dy in range(1, NY):
        hello(barrier, x, z, k, lax.rem(y + dy, NY))

    def ring_signal(r):
        hello(ring.at[r, 0], x, above, k, y)
        hello(ring.at[r, 1], x, below, k, y)

    def ring_wait(r):
        pl.semaphore_wait(ring.at[r, 0], 1)
        pl.semaphore_wait(ring.at[r, 1], 1)

    load_assigned.wait()
    load_slots.wait()
    number = assigned[...].astype(F32)
    at_row = jnp.floor(number * (1.0 / 128.0))
    at_lane = number - at_row * 128.0
    held = slots.shape[0]
    turned = jnp.concatenate(
        [slots[r * 128 : (r + 1) * 128, :].astype(F32).T for r in range(held // 128)], axis=1
    )
    top = jnp.floor(turned * (1.0 / 4096.0))
    turned -= top * 4096.0
    middle = jnp.floor(turned * (1.0 / 64.0))
    turned -= middle * 64.0
    digits = jnp.concatenate([top, middle, turned], axis=0).astype(BF16)
    digits = dot(digits, one_if(fiota((held, count), 0) == at_row, BF16))
    slot = digits[:128] * 4096.0 + digits[128:256] * 64.0 + digits[256:]
    slot = rsum(jnp.where(fiota((128, count), 0) == at_lane, slot, 0.0), 0)

    owner = jnp.floor((slot + 0.5) * (1.0 / table))
    local = slot - owner * table
    row = jnp.floor(owner * (1.0 / NY))
    col = owner - row * NY
    dest_x = jnp.floor(row * (1.0 / (NZ * NK)))
    rest = row - dest_x * (NZ * NK)
    dest_z = jnp.floor(rest * (1.0 / NK))
    dest_k = rest - dest_z * NK
    step = dest_z - z.astype(F32)
    step = jnp.where(step < 0.0, step + NZ, step)
    order = jnp.zeros_like(step)
    for n, dz in enumerate(STEPS):
        order = jnp.where(step == float(dz), float(n), order)
    col = col - y.astype(F32)
    col = jnp.where(col < 0.0, col + NY, col)
    shift_x = dest_x - x.astype(F32)
    shift_x = jnp.where(shift_x < 0.0, shift_x + NX, shift_x)
    shift_k = jnp.abs(dest_k - k.astype(F32))
    turn = shift_x * NK + shift_k
    group = order * NJ + turn
    at_group = one_if(fiota((GROUPS, count), 0) == group)
    at_owner = one_if(fiota((GROUPS * NY, count), 0) == group * NY + col)
    earlier = one_if(iota((count, count), 0) < iota((count, count), 1), BF16)
    rank = rsum(dot(at_group.astype(BF16), earlier) * at_group, 0)
    rank_owner = rsum(dot(at_owner.astype(BF16), earlier) * at_owner, 0)
    is_main = rank < float(MAIN)
    main_at = jnp.where(is_main, group * MAIN + rank, -1.0)
    spill_at = jnp.where(is_main, -8.0, group * MAIN + (rank - MAIN) * 4.0)
    group_ref[...] = group
    place[...] = col * (2.0 * CAP) + rank_owner

    value = col * float(ROWS) + turn * CAP + rank_owner + 1.0
    lane = fiota((128, count), 0)
    main_lane = jnp.where(is_main, turn * MAIN + rank, -8.0)
    spill_lane = jnp.where(is_main, -8.0, 64.0 + turn * MAIN + (rank - MAIN) * 4.0)
    hit = (lane == main_lane) | ((lane >= spill_lane) & (lane < spill_lane + 4.0))
    first = dot(at_group.astype(BF16), jnp.where(hit, value, 0.0).astype(BF16), ((1,), (1,)))
    hit = lane == value - 1.0
    high = jnp.floor((local + 1.0) * (1.0 / 16.0))
    low = local + 1.0 - high * 16.0
    second = 16.0 * dot(at_group.astype(BF16), jnp.where(hit, high, 0.0).astype(BF16), ((1,), (1,)))
    second += dot(at_group.astype(BF16), jnp.where(hit, low, 0.0).astype(BF16), ((1,), (1,)))
    both = jnp.concatenate([first, second], axis=1)
    for g in range(GROUPS):
        tag_out[g] = both[g : g + 1, :]
    tag_in[0] = tag_out[0]

    half = GROUPS // 2

    def pack(h):
        at = fiota((half * MAIN, count), 0) + float(h * half * MAIN)
        pick = one_if(at == main_at, BF16)
        for q in range(4):
            cols = slice(q * quarter, (q + 1) * quarter)
            packed = dot(pick, docs[:, cols]).astype(BF16)
            out[h * half : (h + 1) * half, :, cols] = packed.reshape(half, MAIN, quarter)
        spilled = jnp.zeros((half * MAIN, quarter), F32)
        for q in range(4):
            cols = slice(q * quarter, (q + 1) * quarter)
            spilled += dot(one_if(at == spill_at + float(q), BF16), docs[:, cols])
        out[h * half : (h + 1) * half, :, width:] = spilled.astype(BF16).reshape(half, MAIN, quarter)

    def send(ref_out, ref_in, sems, n, t, sign=1):
        px, pz, pk = peer(STEPS[n], t, sign)
        pltpu.make_async_remote_copy(
            src_ref=ref_out.at[n * NJ + t],
            dst_ref=ref_in.at[n * NJ + t],
            send_sem=sems[0],
            recv_sem=sems[1],
            device_id=(px, pz, pk, y),
            device_id_type=MESH,
        ).start()

    def send_group(ref_out, ref_in, sems, n, sign=1, first=0, last=NJ):
        def body(t, carry):
            send(ref_out, ref_in, sems, n, t, sign)
            return carry

        lax.fori_loop(max(first, 1 if n == 0 else 0), last, body, 0)

    def plane_send(n):
        ref_in, sems = (mid, (hop_send, mid_recv.at[n])) if n else (inbox, (doc_send.at[0], doc_recv.at[0]))

        def body(t, carry):
            px, pz, pk = peer(0, t)
            pltpu.make_async_remote_copy(
                src_ref=out.at[n * NJ + t],
                dst_ref=ref_in.at[n * NJ + t],
                send_sem=sems[0],
                recv_sem=sems[1],
                device_id=(px, pz, pk, y),
                device_id_type=MESH,
            ).start()
            return carry

        lax.fori_loop(1, NJ, body, 0)

    def z_send(n, ref_out, first, many):
        odd = lax.rem(n, 2)
        dz = lax.rem(odd * ((n + 1) // 2) + (1 - odd) * (NZ - n // 2), NZ)
        rows = pl.ds(n * NJ + first, many)
        pltpu.make_async_remote_copy(
            src_ref=ref_out.at[rows],
            dst_ref=inbox.at[rows],
            send_sem=doc_send.at[n],
            recv_sem=doc_recv.at[n + (n // (NZ - 1)) * (first // (NJ // 2))],
            device_id=(x, lax.rem(z + dz, NZ), k, y),
            device_id_type=MESH,
        ).start()

    def z_forward(n):
        arrived(mid.at[pl.ds(0, NJ - 1)], mid_recv.at[n])
        z_send(n, mid, 1, NJ // 2 - 1)
        z_send(n, mid, NJ // 2, NJ // 2)

    def send_tags(n):
        send_group(tag_out, tag_in, (tag_send, tag_recv.at[n]), n)

    def arrived(ref, sem):
        pltpu.make_async_copy(ref, ref, sem).wait()

    def y_send(dy, src, dst, send, recv):
        return pltpu.make_async_remote_copy(
            src_ref=src, dst_ref=dst, send_sem=send, recv_sem=recv,
            device_id=(x, z, k, lax.rem(y + dy, NY)), device_id_type=MESH,
        )

    load_docs.wait()
    pack(0)
    pl.semaphore_wait(barrier, NJ - 1 + NY - 1 + 2)
    ring_signal(0)
    send_tags(0)
    for n in PLANE_FIRST:
        plane_send(n)
    ring_wait(0)
    ring_signal(1)
    for n in (1, 2):
        send_tags(n)
        z_send(n, out, 0, 1)
    inbox[0] = out[0]
    pack(1)
    ring_wait(1)
    ring_signal(2)
    for n in (3, 4):
        send_tags(n)
        z_send(n, out, 0, 1)
    for n in PLANE_THEN:
        plane_send(n)
    ring_wait(2)
    ring_signal(3)
    for n in (5, 6):
        send_tags(n)
        z_send(n, out, 0, 1)
    ring_wait(3)
    send_tags(7)
    z_send(7, out, 0, 1)
    for n in (1, 2, 3, 4):
        z_forward(n)

    tot[...] = jnp.zeros_like(tot)
    best[...] = jnp.zeros_like(best)
    rowbest[...] = jnp.zeros_like(rowbest)

    def relay_tags(n, waited):
        arrived(tag_in.at[pl.ds(0, waited)], tag_recv.at[n])
        own = tag_in[n * NJ]
        for j in range(1, NJ):
            own += tag_in[n * NJ + j]
        own_out[n] = own
        for dy in range(1, NY):
            y_send(dy, own_out.at[n], own_in.at[dy, n], own_send, own_recv.at[n]).start()

    def relay(n, waited, sem, first=0, many=NJ):
        arrived(inbox.at[pl.ds(0, waited)], doc_recv.at[sem])
        marks = own_out[n]
        deep, tall = many * MAIN, many * CAP
        at = iota((NY * tall, deep), 0)
        target = ((at // tall) * ROWS + first * CAP + lax.rem(at, tall) + 1).astype(F32)
        pick = one_if(target == marks[:, first * MAIN : first * MAIN + deep], BF16)
        spill = target == marks[:, 64 + first * MAIN : 64 + first * MAIN + deep]
        phase = lax.rem(iota((NY * tall, deep), 1), 4)
        got = inbox[pl.ds(n * NJ + first, many)].reshape(deep, width + quarter)
        for q in range(4):
            cols = slice(q * quarter, (q + 1) * quarter)
            rows = dot(pick, got[:, cols])
            rows += dot(one_if(spill & (phase == q), BF16), got[:, width:])
            rows = rows.astype(BF16)
            block[n, first * CAP : first * CAP + tall, cols] = rows[:tall]
            for dy in range(1, NY):
                at_row = (dy - 1) * ROWS + first * CAP
                fwd[n, at_row : at_row + tall, cols] = rows[dy * tall : (dy + 1) * tall]
        for dy in range(1, NY):
            y_send(
                dy,
                fwd.at[n, pl.ds((dy - 1) * ROWS + first * CAP, tall)],
                block.at[n, pl.ds(dy * ROWS + first * CAP, tall)],
                fwd_send.at[n],
                fwd_recv.at[n],
            ).start()

    eye = iota((BLOCK, BLOCK), 0) == iota((BLOCK, BLOCK), 1)
    source = iota((1, 128), 1) // ROWS

    def owner_block(n, last=False):
        arrived(block.at[n, pl.ds(0, BLOCK - ROWS)], fwd_recv.at[n])
        mine = block[n]
        arrived(own_out.at[pl.ds(0, NY - 1)], own_recv.at[n])
        tag = own_out[n][:, 128:]
        for dy in range(1, NY):
            tag = jnp.where(source == dy, own_in[dy, n][:, 128:], tag)
        tags[pl.ds(n, 1), :] = tag
        live = tag > 0.0
        gram = dot(mine, mine, ((1,), (1,)))
        square = jnp.where(eye, gram, 0.0)
        scale = lax.rsqrt(rsum(square, 0) + 1.0)
        scale_col = lax.rsqrt(rsum(square, 1) + 1.0)
        tag_col = rsum(jnp.where(eye, jnp.broadcast_to(tag, (BLOCK, BLOCK)), 0.0), 1)
        rowscale[n] = jnp.broadcast_to(scale_col, (BLOCK, BLOCK))
        rowtag[n] = jnp.broadcast_to(tag_col, (BLOCK, BLOCK))
        pair = jnp.where((tag_col == tag) & live & jnp.logical_not(eye), gram, 0.0)
        top = rmax(pair * scale_col, 0)

        def meet(m, other, top):
            pair = jnp.where((rowtag[m] == tag) & live, other, 0.0)
            rowbest[m] = jnp.maximum(rowbest[m], pair * scale)
            return jnp.maximum(top, rmax(pair * rowscale[m], 0))

        if last:
            for begin, end in ((0, 4), (4, NZ - 1)):
                rows = (end - begin) * BLOCK
                others = dot(block[begin:end].reshape(rows, width), mine, ((1,), (1,)))
                for m in range(begin, end):
                    top = meet(m, others[(m - begin) * BLOCK : (m - begin + 1) * BLOCK], top)
        else:

            def earlier_block(m, top):
                return meet(m, dot(block[m], mine, ((1,), (1,))), top)

            top = lax.fori_loop(0, n, earlier_block, top)
        best[pl.ds(n, 1), :] = top * scale

        cross = dot(cents[...], mine, ((1,), (1,)))
        member = (fiota((table, BLOCK), 0) + 1.0) == tag
        similar = rsum(jnp.where(member, cross * qcol[...], 0.0), 0) * scale
        simil[pl.ds(n, 1), :] = similar
        tot[0] += one_if(member)
        tot[1] += jnp.where(member, similar, 0.0)
        tot[2] += jnp.where(member, similar * similar, 0.0)

    load_cents.wait()
    squares = jnp.zeros((table, 128), F32)
    for c in range(width // 128):
        part = cents[:, c * 128 : (c + 1) * 128].astype(F32)
        squares += part * part
    qcol[...] = lax.rsqrt(rsum(squares, 1) + 1.0)


    def main_step(i, carry):
        relay_tags(2 * i + 1, NJ)
        relay(2 * i + 1, NJ, 2 * i + 1)

        @pl.when(i == 0)
        def _():
            for n in (5, 6, 7):
                z_forward(n)

        relay_tags(2 * i + 2, NJ)
        relay(2 * i + 2, NJ, 2 * i + 2)
        @pl.when(i == 0)
        def _():
            relay_tags(0, NJ - 1)
            relay(0, NJ - 1, 0)

        @pl.when(i > 0)
        def _():
            owner_block(2 * i - 2)
            owner_block(2 * i - 1)

        return carry

    lax.fori_loop(0, (NZ - 2) // 2, main_step, 0)
    owner_block(NZ - 4)
    relay_tags(NZ - 1, NJ)
    relay(NZ - 1, NJ // 2, NZ - 1, 0, NJ // 2)
    relay(NZ - 1, NJ // 2, NZ, NJ // 2, NJ // 2)
    owner_block(NZ - 3)
    owner_block(NZ - 2)
    owner_block(NZ - 1, last=True)

    counts = rsum(tot[0], 1)
    sums = rsum(tot[1], 1)
    squares = rsum(tot[2], 1)
    pos = iota((table, 128), 1)
    stacked = jnp.where(pos == 0, counts, jnp.where(pos == 1, sums, jnp.where(pos == 2, squares, 0.0)))
    stats_ref[...] = stacked.T[:3]
    floor = jnp.maximum(counts, 1.0)
    mean = sums / floor
    spread = jnp.sqrt(jnp.maximum(squares / floor - mean * mean, 0.0) + 1.0 / width)

    def scores(n, carry):
        tag = tags[pl.ds(n, 1), :]
        member = (fiota((table, BLOCK), 0) + 1.0) == tag
        mean_at = rsum(jnp.where(member, mean, 0.0), 0)
        spread_at = rsum(jnp.where(member, spread, 0.0), 0)
        gap = (mean_at - simil[pl.ds(n, 1), :]) / jnp.where(tag > 0.0, spread_at, 1.0)
        score[0, pl.ds(n, 1), :] = jnp.where(tag > 0.0, gap, 0.0)
        rows = rmax((rowbest[n] * rowscale[n]).T, 0)
        score[1, pl.ds(n, 1), :] = math.sqrt(width) * jnp.maximum(best[pl.ds(n, 1), :], rows)
        return carry

    lax.fori_loop(0, NZ, scores, 0)
    for dy in range(1, NY):
        y_send(NY - dy, score, score_in.at[dy], score_send, score_recv).start()
    score_in[0] = score[...]

    arrived(score_in.at[pl.ds(1, NY - 1)], score_recv)
    lanes = iota((GROUPS, 128), 1)
    mine = lax.rem(lanes, ROWS) // CAP == lax.rem(iota((GROUPS, 128), 0), NJ)
    from_lane, to_lane = iota((128, 128), 0), iota((128, 128), 1)
    laid = jnp.zeros((GROUPS, 128), F32)
    for s in range(2):
        held = jnp.zeros((NZ, 128), F32)
        for dy in range(NY):
            held = jnp.where(iota((NZ, 128), 1) // ROWS == dy, score_in[dy, s], held)
        held = jnp.broadcast_to(held[:, None, :], (NZ, NJ, 128)).reshape(GROUPS, 128)
        move = one_if(to_lane == (from_lane // ROWS) * (2 * CAP) + s * CAP + lax.rem(from_lane, CAP))
        laid += dot(jnp.where(mine, held, 0.0), move, precision=HIGHEST)
    for g in range(GROUPS):
        reply[g] = laid[g : g + 1, :]

    for n in reversed(range(NZ)):
        send_group(reply, reply_in, (reply_send, reply_recv), n, sign=-1)
    reply_in[0] = reply[0]

    for n, dz in enumerate(STEPS):
        arrived(inbox.at[pl.ds(0, NJ - 1 if dz == 0 else NJ)], doc_send.at[n])
        arrived(fwd.at[n], fwd_send.at[n])
    arrived(tag_out.at[pl.ds(0, GROUPS - 1)], tag_send)
    arrived(inbox.at[pl.ds(0, (NZ - 1) * (NJ - 1))], hop_send)
    for dy in range(1, NY):
        arrived(own_in.at[dy], own_send)
    arrived(score_in.at[pl.ds(1, NY - 1)], score_send)
    arrived(reply.at[pl.ds(0, GROUPS - 1)], reply_send)
    arrived(reply_in.at[pl.ds(0, GROUPS - 1)], reply_recv)


def unpack(reply_ref, group_ref, place, stats_ref, proto_ref, red_ref, totals_ref):
    count = group_ref.shape[1]
    assign = one_if(fiota((GROUPS, count), 0) == group_ref[...])
    home = jnp.concatenate(
        [reply_ref[...].reshape(GROUPS, 128), jnp.zeros((128 - GROUPS, 128), F32)], axis=0
    ).T
    picked = dot(home[: NY * 2 * CAP, :GROUPS], assign, precision=HIGHEST)
    at = fiota((NY * 2 * CAP, count), 0)
    proto_ref[...] = rsum(jnp.where(at == place[...], picked, 0.0), 0)
    red_ref[...] = rsum(jnp.where(at == place[...] + CAP, picked, 0.0), 0)
    totals_ref[...] = stats_ref[...]


def local(documents, assigned, centroids, owner_slot):
    count, width = documents.shape
    table = centroids.shape[0]
    wide = width + width // 4
    dma = pltpu.SemaphoreType.DMA
    outs = (
        jax.ShapeDtypeStruct((1, count), F32),
        jax.ShapeDtypeStruct((1, count), F32),
        jax.ShapeDtypeStruct((3, table), F32),
    )
    vmem = pl.BlockSpec(memory_space=pltpu.VMEM)
    parts = pl.pallas_call(
        kernel,
        out_shape=(
            jax.ShapeDtypeStruct((GROUPS, 1, 128), F32),
            jax.ShapeDtypeStruct((1, count), F32),
            jax.ShapeDtypeStruct((1, count), F32),
            jax.ShapeDtypeStruct((3, table), F32),
        ),
        in_specs=[pl.BlockSpec(memory_space=pl.ANY)] * 4,
        out_specs=(vmem,) * 4,
        scratch_shapes=[
            pltpu.VMEM((1, count), jnp.int32),
            pltpu.VMEM((owner_slot.shape[0] // 128, 128), jnp.int32),
            pltpu.VMEM((count, width), BF16),
            pltpu.VMEM((table, width), BF16),
            pltpu.VMEM((GROUPS, MAIN, wide), BF16),
            pltpu.VMEM((GROUPS, MAIN, wide), BF16),
            pltpu.VMEM((GROUPS, MAIN, wide), BF16),
            pltpu.VMEM((NZ, BLOCK - ROWS, width), BF16),
            pltpu.VMEM((NZ, BLOCK, width), BF16),
            pltpu.VMEM((GROUPS, 1, 256), F32),
            pltpu.VMEM((GROUPS, 1, 256), F32),
            pltpu.VMEM((NZ, 1, 256), F32),
            pltpu.VMEM((NY, NZ, 1, 256), F32),
            pltpu.VMEM((table, 1), F32),
            pltpu.VMEM((NZ, BLOCK), F32),
            pltpu.VMEM((NZ, BLOCK, BLOCK), F32),
            pltpu.VMEM((NZ, BLOCK, BLOCK), F32),
            pltpu.VMEM((NZ, BLOCK), F32),
            pltpu.VMEM((NZ, BLOCK), F32),
            pltpu.VMEM((NZ, BLOCK, BLOCK), F32),
            pltpu.VMEM((3, table, BLOCK), F32),
            pltpu.VMEM((2, NZ, BLOCK), F32),
            pltpu.VMEM((NY, 2, NZ, BLOCK), F32),
            pltpu.VMEM((GROUPS, 1, 128), F32),
            pltpu.SemaphoreType.REGULAR((NZ // 2, 2)),
            dma((4,)),
            dma((NZ,)), dma, dma((NZ,)), dma((NZ + 1,)),
            dma, dma((NZ,)),
            dma, dma((NZ,)),
            dma((NZ,)), dma((NZ,)),
            dma, dma,
            dma, dma,
        ],
        compiler_params=pltpu.CompilerParams(
            collective_id=0, has_side_effects=True, vmem_limit_bytes=56 * 1024 * 1024
        ),
        name="route_and_score",
    )(assigned.reshape(1, count), owner_slot.reshape(-1, 128), documents, centroids)
    proto, red, stats = pl.pallas_call(
        unpack,
        out_shape=outs,
        in_specs=[vmem] * 4,
        out_specs=(vmem,) * 3,
        name="unpack",
    )(*parts)
    return proto.reshape(count), red.reshape(count), stats


def solution(mesh):
    split = Mesh(mesh.devices.reshape(NX, NZ, NK, NY), AXES)
    placed = (P(AXES, None), P(AXES), P(AXES, None), P())
    return jax.shard_map(
        local,
        mesh=split,
        in_specs=placed,
        out_specs=(P(AXES), P(AXES), P(None, AXES)),
        check_vma=False,
    )
```

```python
import math

import jax
import jax.numpy as jnp
from jax import lax
from jax.experimental import pallas as pl
from jax.experimental.pallas import tpu as pltpu
from jax.sharding import Mesh
from jax.sharding import PartitionSpec as P

AXES = ("dp_0", "dp_1", "dp_2", "cent")
MESH = pl.DeviceIdType.MESH
F32 = jnp.float32
BF16 = jnp.bfloat16
HIGHEST = lax.Precision.HIGHEST

NX, NZ, NK, NY = 4, 8, 2, 4
NJ = NX * NK
GROUPS = NZ * NJ
MAIN, SPILL, CAP = 8, 2, 4
STEPS = tuple((n + 1) // 2 if n % 2 else -(n // 2) % NZ for n in range(NZ))
ROWS = NJ * CAP
PLANE_FIRST, PLANE_THEN = (1, 2, 3), (4, 0, 5, 6, 7)
BLOCK = NY * ROWS


def dot(a, b, dims=((1,), (0,)), precision=None):
    return lax.dot_general(a, b, (dims, ((), ())), precision=precision, preferred_element_type=F32)


def iota(shape, dim):
    return lax.broadcasted_iota(jnp.int32, shape, dim)


def fiota(shape, dim):
    return iota(shape, dim).astype(F32)


def rsum(value, axis):
    return jnp.sum(value, axis=axis, keepdims=True)


def rmax(value, axis):
    return jnp.max(value, axis=axis, keepdims=True)


def one_if(mask, dtype=F32):
    return jnp.where(mask, 1.0, 0.0).astype(dtype)


def kernel(
    assigned_hbm, slots_hbm, docs_hbm, cents_hbm,
    reply_in, group_ref, place, stats_ref,
    assigned, slots, docs, cents, out, mid, inbox, fwd, block,
    tag_out, tag_in, own_out, own_in,
    qcol, tags, rowscale, rowtag, simil, best, rowbest, tot,
    score, score_in, reply,
    ring, load_sem, doc_send, hop_send, mid_recv, doc_recv, tag_send, tag_recv, own_send, own_recv,
    fwd_send, fwd_recv, score_send, score_recv, reply_send, reply_recv,
):
    x, z, k, y = (lax.axis_index(a) for a in AXES)
    count, width = docs.shape
    table = cents.shape[0]
    quarter = width // 4

    load_assigned = pltpu.make_async_copy(assigned_hbm, assigned, load_sem.at[2])
    load_slots = pltpu.make_async_copy(slots_hbm, slots, load_sem.at[3])
    load_docs = pltpu.make_async_copy(docs_hbm, docs, load_sem.at[0])
    load_cents = pltpu.make_async_copy(cents_hbm, cents, load_sem.at[1])
    load_assigned.start()
    load_slots.start()
    load_docs.start()
    load_cents.start()

    def peer(dz, t, sign=1):
        px = lax.rem(x + NX + sign * (t // NK), NX)
        pk = lax.rem(k + NK + sign * lax.rem(t, NK), NK)
        pz = lax.rem(z + NZ + sign * dz, NZ)
        return px, pz, pk

    barrier = pltpu.get_barrier_semaphore()

    def hello(sem, px, pz, pk, py):
        pl.semaphore_signal(sem, inc=1, device_id=(px, pz, pk, py), device_id_type=MESH)

    above, below = lax.rem(z + 1, NZ), lax.rem(z + NZ - 1, NZ)
    hello(barrier, x, above, k, y)
    hello(barrier, x, below, k, y)
    for t in range(1, NJ):
        px, pz, pk = peer(0, t)
        hello(barrier, px, pz, pk, y)
    for dy in range(1, NY):
        hello(barrier, x, z, k, lax.rem(y + dy, NY))

    def ring_signal(r):
        hello(ring.at[r, 0], x, above, k, y)
        hello(ring.at[r, 1], x, below, k, y)

    def ring_wait(r):
        pl.semaphore_wait(ring.at[r, 0], 1)
        pl.semaphore_wait(ring.at[r, 1], 1)

    load_assigned.wait()
    load_slots.wait()
    number = assigned[...].astype(F32)
    at_row = jnp.floor(number * (1.0 / 128.0))
    at_lane = number - at_row * 128.0
    held = slots.shape[0]
    turned = jnp.concatenate(
        [slots[r * 128 : (r + 1) * 128, :].astype(F32).T for r in range(held // 128)], axis=1
    )
    top = jnp.floor(turned * (1.0 / 4096.0))
    turned -= top * 4096.0
    middle = jnp.floor(turned * (1.0 / 64.0))
    turned -= middle * 64.0
    digits = jnp.concatenate([top, middle, turned], axis=0).astype(BF16)
    digits = dot(digits, one_if(fiota((held, count), 0) == at_row, BF16))
    slot = digits[:128] * 4096.0 + digits[128:256] * 64.0 + digits[256:]
    slot = rsum(jnp.where(fiota((128, count), 0) == at_lane, slot, 0.0), 0)

    owner = jnp.floor((slot + 0.5) * (1.0 / table))
    local = slot - owner * table
    row = jnp.floor(owner * (1.0 / NY))
    col = owner - row * NY
    dest_x = jnp.floor(row * (1.0 / (NZ * NK)))
    rest = row - dest_x * (NZ * NK)
    dest_z = jnp.floor(rest * (1.0 / NK))
    dest_k = rest - dest_z * NK
    step = dest_z - z.astype(F32)
    step = jnp.where(step < 0.0, step + NZ, step)
    order = jnp.zeros_like(step)
    for n, dz in enumerate(STEPS):
        order = jnp.where(step == float(dz), float(n), order)
    col = col - y.astype(F32)
    col = jnp.where(col < 0.0, col + NY, col)
    shift_x = dest_x - x.astype(F32)
    shift_x = jnp.where(shift_x < 0.0, shift_x + NX, shift_x)
    shift_k = jnp.abs(dest_k - k.astype(F32))
    turn = shift_x * NK + shift_k
    group = order * NJ + turn
    at_group = one_if(fiota((GROUPS, count), 0) == group)
    at_owner = one_if(fiota((GROUPS * NY, count), 0) == group * NY + col)
    earlier = one_if(iota((count, count), 0) < iota((count, count), 1), BF16)
    rank = rsum(dot(at_group.astype(BF16), earlier) * at_group, 0)
    rank_owner = rsum(dot(at_owner.astype(BF16), earlier) * at_owner, 0)
    is_main = rank < float(MAIN)
    main_at = jnp.where(is_main, group * MAIN + rank, -1.0)
    spill_at = jnp.where(is_main, -8.0, group * MAIN + (rank - MAIN) * 4.0)
    group_ref[...] = group
    place[...] = col * (2.0 * CAP) + rank_owner

    value = col * float(ROWS) + turn * CAP + rank_owner + 1.0
    lane = fiota((128, count), 0)
    main_lane = jnp.where(is_main, turn * MAIN + rank, -8.0)
    spill_lane = jnp.where(is_main, -8.0, 64.0 + turn * MAIN + (rank - MAIN) * 4.0)
    hit = (lane == main_lane) | ((lane >= spill_lane) & (lane < spill_lane + 4.0))
    first = dot(at_group.astype(BF16), jnp.where(hit, value, 0.0).astype(BF16), ((1,), (1,)))
    hit = lane == value - 1.0
    high = jnp.floor((local + 1.0) * (1.0 / 16.0))
    low = local + 1.0 - high * 16.0
    second = 16.0 * dot(at_group.astype(BF16), jnp.where(hit, high, 0.0).astype(BF16), ((1,), (1,)))
    second += dot(at_group.astype(BF16), jnp.where(hit, low, 0.0).astype(BF16), ((1,), (1,)))
    both = jnp.concatenate([first, second], axis=1)
    for g in range(GROUPS):
        tag_out[g] = both[g : g + 1, :]
    tag_in[0] = tag_out[0]

    half = GROUPS // 2

    def pack(h):
        at = fiota((half * MAIN, count), 0) + float(h * half * MAIN)
        pick = one_if(at == main_at, BF16)
        for q in range(4):
            cols = slice(q * quarter, (q + 1) * quarter)
            packed = dot(pick, docs[:, cols]).astype(BF16)
            out[h * half : (h + 1) * half, :, cols] = packed.reshape(half, MAIN, quarter)
        spilled = jnp.zeros((half * MAIN, quarter), F32)
        for q in range(4):
            cols = slice(q * quarter, (q + 1) * quarter)
            spilled += dot(one_if(at == spill_at + float(q), BF16), docs[:, cols])
        out[h * half : (h + 1) * half, :, width:] = spilled.astype(BF16).reshape(half, MAIN, quarter)

    def send(ref_out, ref_in, sems, n, t, sign=1):
        px, pz, pk = peer(STEPS[n], t, sign)
        pltpu.make_async_remote_copy(
            src_ref=ref_out.at[n * NJ + t],
            dst_ref=ref_in.at[n * NJ + t],
            send_sem=sems[0],
            recv_sem=sems[1],
            device_id=(px, pz, pk, y),
            device_id_type=MESH,
        ).start()

    def send_group(ref_out, ref_in, sems, n, sign=1, first=0, last=NJ):
        def body(t, carry):
            send(ref_out, ref_in, sems, n, t, sign)
            return carry

        lax.fori_loop(max(first, 1 if n == 0 else 0), last, body, 0)

    def plane_send(n):
        ref_in, sems = (mid, (hop_send, mid_recv.at[n])) if n else (inbox, (doc_send.at[0], doc_recv.at[0]))

        def body(t, carry):
            px, pz, pk = peer(0, t)
            pltpu.make_async_remote_copy(
                src_ref=out.at[n * NJ + t],
                dst_ref=ref_in.at[n * NJ + t],
                send_sem=sems[0],
                recv_sem=sems[1],
                device_id=(px, pz, pk, y),
                device_id_type=MESH,
            ).start()
            return carry

        lax.fori_loop(1, NJ, body, 0)

    def z_send(n, ref_out, first, many):
        odd = lax.rem(n, 2)
        dz = lax.rem(odd * ((n + 1) // 2) + (1 - odd) * (NZ - n // 2), NZ)
        rows = pl.ds(n * NJ + first, many)
        pltpu.make_async_remote_copy(
            src_ref=ref_out.at[rows],
            dst_ref=inbox.at[rows],
            send_sem=doc_send.at[n],
            recv_sem=doc_recv.at[n + (n // (NZ - 1)) * (first // (NJ // 2))],
            device_id=(x, lax.rem(z + dz, NZ), k, y),
            device_id_type=MESH,
        ).start()

    def z_forward(n):
        arrived(mid.at[pl.ds(0, NJ - 1)], mid_recv.at[n])
        z_send(n, mid, 1, NJ // 2 - 1)
        z_send(n, mid, NJ // 2, NJ // 2)

    def send_tags(n):
        send_group(tag_out, tag_in, (tag_send, tag_recv.at[n]), n)

    def arrived(ref, sem):
        pltpu.make_async_copy(ref, ref, sem).wait()

    def y_send(dy, src, dst, send, recv):
        return pltpu.make_async_remote_copy(
            src_ref=src, dst_ref=dst, send_sem=send, recv_sem=recv,
            device_id=(x, z, k, lax.rem(y + dy, NY)), device_id_type=MESH,
        )

    load_docs.wait()
    pack(0)
    pl.semaphore_wait(barrier, NJ - 1 + NY - 1 + 2)
    ring_signal(0)
    send_tags(0)
    for n in PLANE_FIRST:
        plane_send(n)
    ring_wait(0)
    ring_signal(1)
    for n in (1, 2):
        send_tags(n)
        z_send(n, out, 0, 1)
    inbox[0] = out[0]
    pack(1)
    ring_wait(1)
    ring_signal(2)
    for n in (3, 4):
        send_tags(n)
        z_send(n, out, 0, 1)
    for n in PLANE_THEN:
        plane_send(n)
    ring_wait(2)
    ring_signal(3)
    for n in (5, 6):
        send_tags(n)
        z_send(n, out, 0, 1)
    ring_wait(3)
    send_tags(7)
    z_send(7, out, 0, 1)
    for n in (1, 2, 3, 4):
        z_forward(n)

    tot[...] = jnp.zeros_like(tot)
    best[...] = jnp.zeros_like(best)
    rowbest[...] = jnp.zeros_like(rowbest)

    def relay_tags(n, waited):
        arrived(tag_in.at[pl.ds(0, waited)], tag_recv.at[n])
        own = tag_in[n * NJ]
        for j in range(1, NJ):
            own += tag_in[n * NJ + j]
        own_out[n] = own
        for dy in range(1, NY):
            y_send(dy, own_out.at[n], own_in.at[dy, n], own_send, own_recv.at[n]).start()

    def relay(n, waited, sem, first=0, many=NJ):
        arrived(inbox.at[pl.ds(0, waited)], doc_recv.at[sem])
        marks = own_out[n]
        deep, tall = many * MAIN, many * CAP
        at = iota((NY * tall, deep), 0)
        target = ((at // tall) * ROWS + first * CAP + lax.rem(at, tall) + 1).astype(F32)
        pick = one_if(target == marks[:, first * MAIN : first * MAIN + deep], BF16)
        spill = target == marks[:, 64 + first * MAIN : 64 + first * MAIN + deep]
        phase = lax.rem(iota((NY * tall, deep), 1), 4)
        got = inbox[pl.ds(n * NJ + first, many)].reshape(deep, width + quarter)
        for q in range(4):
            cols = slice(q * quarter, (q + 1) * quarter)
            rows = dot(pick, got[:, cols])
            rows += dot(one_if(spill & (phase == q), BF16), got[:, width:])
            rows = rows.astype(BF16)
            block[n, first * CAP : first * CAP + tall, cols] = rows[:tall]
            for dy in range(1, NY):
                at_row = (dy - 1) * ROWS + first * CAP
                fwd[n, at_row : at_row + tall, cols] = rows[dy * tall : (dy + 1) * tall]
        for dy in (2, 1, 3):
            y_send(
                dy,
                fwd.at[n, pl.ds((dy - 1) * ROWS + first * CAP, tall)],
                block.at[n, pl.ds(dy * ROWS + first * CAP, tall)],
                fwd_send.at[n],
                fwd_recv.at[n],
            ).start()

    eye = iota((BLOCK, BLOCK), 0) == iota((BLOCK, BLOCK), 1)
    source = iota((1, 128), 1) // ROWS

    def owner_block(n, last=False):
        arrived(block.at[n, pl.ds(0, BLOCK - ROWS)], fwd_recv.at[n])
        mine = block[n]
        arrived(own_out.at[pl.ds(0, NY - 1)], own_recv.at[n])
        tag = own_out[n][:, 128:]
        for dy in range(1, NY):
            tag = jnp.where(source == dy, own_in[dy, n][:, 128:], tag)
        tags[pl.ds(n, 1), :] = tag
        live = tag > 0.0
        gram = dot(mine, mine, ((1,), (1,)))
        square = jnp.where(eye, gram, 0.0)
        scale = lax.rsqrt(rsum(square, 0) + 1.0)
        scale_col = lax.rsqrt(rsum(square, 1) + 1.0)
        tag_col = rsum(jnp.where(eye, jnp.broadcast_to(tag, (BLOCK, BLOCK)), 0.0), 1)
        rowscale[n] = jnp.broadcast_to(scale_col, (BLOCK, BLOCK))
        rowtag[n] = jnp.broadcast_to(tag_col, (BLOCK, BLOCK))
        pair = jnp.where((tag_col == tag) & live & jnp.logical_not(eye), gram, 0.0)
        top = rmax(pair * scale_col, 0)

        def meet(m, other, top):
            pair = jnp.where((rowtag[m] == tag) & live, other, 0.0)
            rowbest[m] = jnp.maximum(rowbest[m], pair * scale)
            return jnp.maximum(top, rmax(pair * rowscale[m], 0))

        if last:
            for begin, end in ((0, 4), (4, NZ - 1)):
                rows = (end - begin) * BLOCK
                others = dot(block[begin:end].reshape(rows, width), mine, ((1,), (1,)))
                for m in range(begin, end):
                    top = meet(m, others[(m - begin) * BLOCK : (m - begin + 1) * BLOCK], top)
        else:

            def earlier_block(m, top):
                return meet(m, dot(block[m], mine, ((1,), (1,))), top)

            top = lax.fori_loop(0, n, earlier_block, top)
        best[pl.ds(n, 1), :] = top * scale

        cross = dot(cents[...], mine, ((1,), (1,)))
        member = (fiota((table, BLOCK), 0) + 1.0) == tag
        similar = rsum(jnp.where(member, cross * qcol[...], 0.0), 0) * scale
        simil[pl.ds(n, 1), :] = similar
        tot[0] += one_if(member)
        tot[1] += jnp.where(member, similar, 0.0)
        tot[2] += jnp.where(member, similar * similar, 0.0)

    load_cents.wait()
    squares = jnp.zeros((table, 128), F32)
    for c in range(width // 128):
        part = cents[:, c * 128 : (c + 1) * 128].astype(F32)
        squares += part * part
    qcol[...] = lax.rsqrt(rsum(squares, 1) + 1.0)


    def main_step(i, carry):
        relay_tags(2 * i + 1, NJ)
        relay(2 * i + 1, NJ, 2 * i + 1)

        @pl.when(i == 0)
        def _():
            for n in (5, 6, 7):
                z_forward(n)

        relay_tags(2 * i + 2, NJ)
        relay(2 * i + 2, NJ, 2 * i + 2)
        @pl.when(i == 0)
        def _():
            relay_tags(0, NJ - 1)
            relay(0, NJ - 1, 0)

        @pl.when(i > 0)
        def _():
            owner_block(2 * i - 2)
            owner_block(2 * i - 1)

        return carry

    lax.fori_loop(0, (NZ - 2) // 2, main_step, 0)
    owner_block(NZ - 4)
    relay_tags(NZ - 1, NJ)
    relay(NZ - 1, NJ // 2, NZ - 1, 0, NJ // 2)
    relay(NZ - 1, NJ // 2, NZ, NJ // 2, NJ // 2)
    owner_block(NZ - 3)
    owner_block(NZ - 2)
    owner_block(NZ - 1, last=True)

    counts = rsum(tot[0], 1)
    sums = rsum(tot[1], 1)
    squares = rsum(tot[2], 1)
    floor = jnp.maximum(counts, 1.0)
    mean = sums / floor
    spread = jnp.sqrt(jnp.maximum(squares / floor - mean * mean, 0.0) + 1.0 / width)

    def scores(n, carry):
        tag = tags[pl.ds(n, 1), :]
        member = (fiota((table, BLOCK), 0) + 1.0) == tag
        mean_at = rsum(jnp.where(member, mean, 0.0), 0)
        spread_at = rsum(jnp.where(member, spread, 0.0), 0)
        gap = (mean_at - simil[pl.ds(n, 1), :]) / jnp.where(tag > 0.0, spread_at, 1.0)
        score[0, pl.ds(n, 1), :] = jnp.where(tag > 0.0, gap, 0.0)
        rows = rmax((rowbest[n] * rowscale[n]).T, 0)
        score[1, pl.ds(n, 1), :] = math.sqrt(width) * jnp.maximum(best[pl.ds(n, 1), :], rows)
        return carry

    lax.fori_loop(0, NZ, scores, 0)
    for dy in range(1, NY):
        y_send(NY - dy, score, score_in.at[dy], score_send, score_recv).start()
    score_in[0] = score[...]
    pos = iota((table, 128), 1)
    stacked = jnp.where(pos == 0, counts, jnp.where(pos == 1, sums, jnp.where(pos == 2, squares, 0.0)))
    stats_ref[...] = stacked.T[:3]

    arrived(score_in.at[pl.ds(1, NY - 1)], score_recv)
    lanes = iota((GROUPS, 128), 1)
    mine = lax.rem(lanes, ROWS) // CAP == lax.rem(iota((GROUPS, 128), 0), NJ)
    from_lane, to_lane = iota((128, 128), 0), iota((128, 128), 1)
    laid = jnp.zeros((GROUPS, 128), F32)
    for s in range(2):
        held = jnp.zeros((NZ, 128), F32)
        for dy in range(NY):
            held = jnp.where(iota((NZ, 128), 1) // ROWS == dy, score_in[dy, s], held)
        held = jnp.broadcast_to(held[:, None, :], (NZ, NJ, 128)).reshape(GROUPS, 128)
        move = one_if(to_lane == (from_lane // ROWS) * (2 * CAP) + s * CAP + lax.rem(from_lane, CAP))
        laid += dot(jnp.where(mine, held, 0.0), move, precision=HIGHEST)
    for g in range(GROUPS):
        reply[g] = laid[g : g + 1, :]

    for n in reversed(range(NZ)):
        send_group(reply, reply_in, (reply_send, reply_recv), n, sign=-1)
    reply_in[0] = reply[0]

    for n, dz in enumerate(STEPS):
        arrived(inbox.at[pl.ds(0, NJ - 1 if dz == 0 else NJ)], doc_send.at[n])
        arrived(fwd.at[n], fwd_send.at[n])
    arrived(tag_out.at[pl.ds(0, GROUPS - 1)], tag_send)
    arrived(inbox.at[pl.ds(0, (NZ - 1) * (NJ - 1))], hop_send)
    for dy in range(1, NY):
        arrived(own_in.at[dy], own_send)
    arrived(score_in.at[pl.ds(1, NY - 1)], score_send)
    arrived(reply.at[pl.ds(0, GROUPS - 1)], reply_send)
    arrived(reply_in.at[pl.ds(0, GROUPS - 1)], reply_recv)


def unpack(reply_ref, group_ref, place, stats_ref, proto_ref, red_ref, totals_ref):
    count = group_ref.shape[1]
    assign = one_if(fiota((GROUPS, count), 0) == group_ref[...])
    home = jnp.concatenate(
        [reply_ref[...].reshape(GROUPS, 128), jnp.zeros((128 - GROUPS, 128), F32)], axis=0
    ).T
    picked = dot(home[: NY * 2 * CAP, :GROUPS], assign, precision=HIGHEST)
    at = fiota((NY * 2 * CAP, count), 0)
    proto_ref[...] = rsum(jnp.where(at == place[...], picked, 0.0), 0)
    red_ref[...] = rsum(jnp.where(at == place[...] + CAP, picked, 0.0), 0)
    totals_ref[...] = stats_ref[...]


def local(documents, assigned, centroids, owner_slot):
    count, width = documents.shape
    table = centroids.shape[0]
    wide = width + width // 4
    dma = pltpu.SemaphoreType.DMA
    outs = (
        jax.ShapeDtypeStruct((1, count), F32),
        jax.ShapeDtypeStruct((1, count), F32),
        jax.ShapeDtypeStruct((3, table), F32),
    )
    vmem = pl.BlockSpec(memory_space=pltpu.VMEM)
    parts = pl.pallas_call(
        kernel,
        out_shape=(
            jax.ShapeDtypeStruct((GROUPS, 1, 128), F32),
            jax.ShapeDtypeStruct((1, count), F32),
            jax.ShapeDtypeStruct((1, count), F32),
            jax.ShapeDtypeStruct((3, table), F32),
        ),
        in_specs=[pl.BlockSpec(memory_space=pl.ANY)] * 4,
        out_specs=(vmem,) * 4,
        scratch_shapes=[
            pltpu.VMEM((1, count), jnp.int32),
            pltpu.VMEM((owner_slot.shape[0] // 128, 128), jnp.int32),
            pltpu.VMEM((count, width), BF16),
            pltpu.VMEM((table, width), BF16),
            pltpu.VMEM((GROUPS, MAIN, wide), BF16),
            pltpu.VMEM((GROUPS, MAIN, wide), BF16),
            pltpu.VMEM((GROUPS, MAIN, wide), BF16),
            pltpu.VMEM((NZ, BLOCK - ROWS, width), BF16),
            pltpu.VMEM((NZ, BLOCK, width), BF16),
            pltpu.VMEM((GROUPS, 1, 256), F32),
            pltpu.VMEM((GROUPS, 1, 256), F32),
            pltpu.VMEM((NZ, 1, 256), F32),
            pltpu.VMEM((NY, NZ, 1, 256), F32),
            pltpu.VMEM((table, 1), F32),
            pltpu.VMEM((NZ, BLOCK), F32),
            pltpu.VMEM((NZ, BLOCK, BLOCK), F32),
            pltpu.VMEM((NZ, BLOCK, BLOCK), F32),
            pltpu.VMEM((NZ, BLOCK), F32),
            pltpu.VMEM((NZ, BLOCK), F32),
            pltpu.VMEM((NZ, BLOCK, BLOCK), F32),
            pltpu.VMEM((3, table, BLOCK), F32),
            pltpu.VMEM((2, NZ, BLOCK), F32),
            pltpu.VMEM((NY, 2, NZ, BLOCK), F32),
            pltpu.VMEM((GROUPS, 1, 128), F32),
            pltpu.SemaphoreType.REGULAR((NZ // 2, 2)),
            dma((4,)),
            dma((NZ,)), dma, dma((NZ,)), dma((NZ + 1,)),
            dma, dma((NZ,)),
            dma, dma((NZ,)),
            dma((NZ,)), dma((NZ,)),
            dma, dma,
            dma, dma,
        ],
        compiler_params=pltpu.CompilerParams(
            collective_id=0, has_side_effects=True, vmem_limit_bytes=56 * 1024 * 1024
        ),
        name="route_and_score",
    )(assigned.reshape(1, count), owner_slot.reshape(-1, 128), documents, centroids)
    proto, red, stats = pl.pallas_call(
        unpack,
        out_shape=outs,
        in_specs=[vmem] * 4,
        out_specs=(vmem,) * 3,
        name="unpack",
    )(*parts)
    return proto.reshape(count), red.reshape(count), stats


def solution(mesh):
    split = Mesh(mesh.devices.reshape(NX, NZ, NK, NY), AXES)
    placed = (P(AXES, None), P(AXES), P(AXES, None), P())
    return jax.shard_map(
        local,
        mesh=split,
        in_specs=placed,
        out_specs=(P(AXES), P(AXES), P(None, AXES)),
        check_vma=False,
    )
```
